128 devices in a mesh: row: 16 (over x, y), col: 8 (over z, core).
Axes of the slice: x: 4, y: 4, z: 4, core: 2. Of those that a mesh axis runs over, the one named last changes fastest.
Arguments:
- mask: float32 [8192, 8192], P('row', 'col'), may hold values from -6 to 6
- target: bfloat16 [8192, 8192], P('row', 'col'), may hold values from 0 to 1
- live: int32 [16, 16], P('row', 'col'), may hold values from 0 to 1, as said below
- pupils: float32 [2, 12, 144, 144], replicated, may hold values from -8 to 8
- weights: float32 [12], replicated, may hold values from 0.1 to 1
Outputs:
- updated_mask: float32 [8192, 8192], P('row', 'col')
The draws below stay inside these ranges and needn't reach their ends.
Inputs may be any that keep to these rules, and one draw needn't show every extreme that they name: In each tile row exactly 5 tiles are live and the others are 0; all 2 tiles of at least one device of the row are live.
All inputs are finite; a program needn't handle non-finite values.
Results may differ from the reference program's by a relative error of at most 0.013.
Values may be sent and summed in bfloat16 or wider, within the bound.
A program may use at most 128 MiB of HBM per device.

```python
import math
import jax
import jax.numpy as jnp
from jax import lax

TILE = 512
AMBIT = 128
KC = 144
KERNELS = 12
SLOTS = 2
TROWS = 16
GROUP = 8
TCOLS = 16
LIVE_ROW = 5
HEIGHT = 8192
WIDTH = 8192


def draw_live(key, part):
    key_scores, key_holder = jax.random.split(key)
    columns = jnp.arange(TCOLS, dtype=jnp.int32)
    scores = jax.random.randint(key_scores, (TROWS, TCOLS), 0, 1 << 20, dtype=jnp.int32) * TCOLS + columns[None, :]
    chosen = jax.random.randint(key_holder, (TROWS, 1), 0, GROUP, dtype=jnp.int32)
    holder = columns[None, :] // SLOTS
    scores = scores + jnp.where(holder == chosen, 1 << 26, 0).astype(jnp.int32)
    cutoff = lax.top_k(scores, LIVE_ROW)[0][:, -1:]
    return (scores >= cutoff).astype(jnp.int32)


def shard_levels(own_key, shape, shards, least, largest):
    loudness, own = 1.0, jax.random.fold_in(own_key, 6)
    for dim, parts in shards:
        steps = jnp.exp(jax.random.uniform(jax.random.fold_in(own, dim), (parts,), jnp.float32, least / len(shards), largest / len(shards)))
        loudness = loudness * jnp.repeat(steps, shape[dim] // parts).reshape([-1 if axis == dim else 1 for axis in range(len(shape))])
    return loudness


def gaussian(stream_key, shape, width, bound, cuts=(), held_as=jnp.bfloat16):
    values = width * jax.random.normal(stream_key, shape, jnp.float32)
    if cuts:
        values = values * shard_levels(stream_key, shape, cuts, -0.22, 0.18)
    return jnp.clip(values, -bound, bound).astype(held_as)


def setup_inputs(seed: int = 0) -> dict:
    arg_keys = jax.random.split(jax.random.key(seed), 6)
    mask = gaussian(arg_keys[0], (HEIGHT, WIDTH), 1.0, 6.0, ((0, 16), (1, 8)), jnp.float32)
    target = jnp.clip(1.0 * jax.random.uniform(arg_keys[1], (HEIGHT, WIDTH), jnp.float32) ** shard_levels(arg_keys[1], (HEIGHT, WIDTH), ((0, 16), (1, 8)), -0.2, 0.2), 0.0, 1.0).astype(jnp.bfloat16)
    live = draw_live(jax.random.fold_in(arg_keys[5], 71), 0)
    pupils = gaussian(arg_keys[3], (2, KERNELS, KC, KC), 1.75, 8.0, (), jnp.float32)
    weights = jnp.clip(jnp.exp(jax.random.uniform(arg_keys[4], (KERNELS,), jnp.float32, math.log(0.1), math.log(1.0))), 0.1, 1.0)
    return dict(mask=mask, target=target, live=live, pupils=pupils, weights=weights)


steepness = 4.0
threshold_level = 1.0
step_rate = 8.0

def matmul(leading, trailing):
    return jnp.dot(leading, trailing, preferred_element_type=jnp.float32)

def contract_first(leading, trailing):
    return lax.dot_general(leading, trailing, (((0,), (0,)), ((), ())), preferred_element_type=jnp.float32)

def contract_last(leading, trailing):
    return lax.dot_general(leading, trailing, (((1,), (1,)), ((), ())), preferred_element_type=jnp.float32)

def cosine_pair(freq_count, pixel_count, offset, period):
    frequency = jnp.arange(freq_count, dtype=jnp.int32) - freq_count // 2
    pixels = jnp.arange(pixel_count, dtype=jnp.int32) + offset
    phases = jnp.mod(frequency[:, None] * pixels[None, :], period).astype(jnp.float32)
    angles = phases * (2.0 * math.pi / period)
    factor = 1.0 / math.sqrt(period)
    return ((jnp.cos(angles) * factor).astype(jnp.bfloat16), (jnp.sin(angles) * factor).astype(jnp.bfloat16))

def transform_tables(spectrum_size, tile_size, ambit_size):
    extent = tile_size + 2 * ambit_size
    outer_cos, outer_sin = cosine_pair(spectrum_size, extent, 0, extent)
    forward = jnp.concatenate([outer_cos, outer_sin], axis=0)
    inner_cos, inner_sin = cosine_pair(spectrum_size, tile_size, ambit_size, extent)
    inverse = jnp.concatenate([inner_cos, inner_sin], axis=0)
    rotate = jnp.concatenate([jnp.concatenate([inner_cos, inner_sin], axis=1), jnp.concatenate([-inner_sin, inner_cos], axis=1)], axis=0)
    return (forward, inverse, rotate)

def spectrum(extended, forward):
    spectrum_size = forward.shape[0] // 2
    partial_rows = matmul(forward, extended).astype(jnp.bfloat16)
    blocks = contract_last(partial_rows, forward)
    real_spectrum = blocks[:spectrum_size, :spectrum_size] - blocks[spectrum_size:, spectrum_size:]
    imaginary_spectrum = -(blocks[:spectrum_size, spectrum_size:] + blocks[spectrum_size:, :spectrum_size])
    return jnp.stack([real_spectrum, imaginary_spectrum]).astype(jnp.bfloat16)

def spectral_gradient(spectra, goal_tile, live_flag, pupils, weights, inverse, rotate):
    real_spectrum = spectra[0].astype(jnp.float32)
    imaginary_spectrum = spectra[1].astype(jnp.float32)
    tile_size = inverse.shape[1]
    spectrum_size = real_spectrum.shape[0]

    def forward_kernel(intensity, inputs):
        pupil_real, pupil_imaginary, weight = inputs
        wave_real = pupil_real * real_spectrum - pupil_imaginary * imaginary_spectrum
        wave_imaginary = pupil_real * imaginary_spectrum + pupil_imaginary * real_spectrum
        amplitude = jnp.concatenate([jnp.concatenate([wave_real, -wave_imaginary], axis=1), jnp.concatenate([wave_imaginary, wave_real], axis=1)], axis=0).astype(jnp.bfloat16)
        section_one = matmul(amplitude, inverse).astype(jnp.bfloat16)
        field_pair = contract_first(rotate, section_one)
        energy = field_pair[:tile_size] ** 2 + field_pair[tile_size:] ** 2
        return (intensity + weight * energy, field_pair.astype(jnp.bfloat16))
    initial = jnp.zeros((tile_size, tile_size), jnp.float32)
    intensity, fields = lax.scan(forward_kernel, initial, (pupils[0], pupils[1], weights))
    resist = jax.nn.sigmoid(steepness * (intensity - threshold_level))
    slope_map = live_flag * (resist - goal_tile.astype(jnp.float32)) * steepness * resist * (1.0 - resist)
    doubled = jnp.concatenate([slope_map, slope_map], axis=0)

    def backward_kernel(totals, inputs):
        pupil_real, pupil_imaginary, weight, field_pair = inputs
        cotangent = (2.0 * weight * doubled * field_pair.astype(jnp.float32)).astype(jnp.bfloat16)
        section_back = matmul(rotate, cotangent).astype(jnp.bfloat16)
        wave_back = contract_last(section_back, inverse)
        adjoint_real = wave_back[:spectrum_size, :spectrum_size] + wave_back[spectrum_size:, spectrum_size:]
        adjoint_imaginary = wave_back[spectrum_size:, :spectrum_size] - wave_back[:spectrum_size, spectrum_size:]
        total_real = totals[0] + pupil_real * adjoint_real + pupil_imaginary * adjoint_imaginary
        total_imaginary = totals[1] - pupil_imaginary * adjoint_real + pupil_real * adjoint_imaginary
        return ((total_real, total_imaginary), None)
    empty_spec = jnp.zeros((spectrum_size, spectrum_size), jnp.float32)
    sums, unused = lax.scan(backward_kernel, (empty_spec, empty_spec), (pupils[0], pupils[1], weights, fields))
    return jnp.stack([sums[0], sums[1]]).astype(jnp.bfloat16)

def pixel_gradient(gradient, forward):
    adjoint_real = gradient[0]
    adjoint_imaginary = gradient[1]
    upper_rows = jnp.concatenate([adjoint_real, -adjoint_imaginary], axis=1)
    lower_rows = jnp.concatenate([-adjoint_imaginary, -adjoint_real], axis=1)
    blocks = jnp.concatenate([upper_rows, lower_rows], axis=0)
    partial_rows = matmul(blocks, forward).astype(jnp.bfloat16)
    return contract_first(forward, partial_rows)

def tile_gradient(extended, goal_tile, live_flag, pupils, weights, forward, inverse, rotate):
    spectra = spectrum(extended, forward)
    gradient = spectral_gradient(spectra, goal_tile, live_flag, pupils, weights, inverse, rotate)
    return pixel_gradient(gradient, forward)

def reference(mask, target, live, pupils, weights):
    forward, inverse, rotate = transform_tables(KC, TILE, AMBIT)
    padded = jnp.pad(mask.astype(jnp.bfloat16), AMBIT)
    tile_rows = live.shape[0]
    tile_cols = live.shape[1]
    extent = TILE + 2 * AMBIT

    def one_tile(total, index):
        row_index = (index // tile_cols).astype(jnp.int32)
        col_index = (index % tile_cols).astype(jnp.int32)
        row_start = (row_index * TILE).astype(jnp.int32)
        col_start = (col_index * TILE).astype(jnp.int32)
        extended = lax.dynamic_slice(padded, (row_start, col_start), (extent, extent))
        goal_tile = lax.dynamic_slice(target, (row_start, col_start), (TILE, TILE))
        live_flag = live[row_index, col_index]

        def compute():
            return tile_gradient(extended, goal_tile, live_flag.astype(jnp.float32), pupils, weights, forward, inverse, rotate)

        def skipped():
            return jnp.zeros((extent, extent), jnp.float32)
        piece = lax.cond(live_flag > 0, compute, skipped)
        current = lax.dynamic_slice(total, (row_start, col_start), (extent, extent))
        return (lax.dynamic_update_slice(total, current + piece, (row_start, col_start)), None)
    initial = jnp.zeros(padded.shape, jnp.float32)
    total, unused = lax.scan(one_tile, initial, jnp.arange(tile_rows * tile_cols, dtype=jnp.int32))
    gradient = total[AMBIT:AMBIT + mask.shape[0], AMBIT:AMBIT + mask.shape[1]]
    return mask - step_rate * gradient
```

```python
from functools import partial
import math

import jax
import jax.numpy as jnp
import numpy as np
from jax import lax
from jax.experimental import pallas as pl
from jax.experimental.pallas import tpu as pltpu
from jax.sharding import PartitionSpec as P

AMBIT = 128
ROWS = 80
LANES = 128

steepness = 4.0
threshold_level = 1.0
step_rate = 8.0


def folded(count, pixels, offset, period, pad):
    half = count // 2
    frequency = np.arange(half + 1)
    place = np.arange(pixels) + offset
    phases = np.mod(frequency[:, None] * place[None, :], period).astype(np.float32)
    angles = phases * np.float32(2.0 * math.pi / period)
    factor = np.float32(1.0 / math.sqrt(period))
    table = np.zeros((2, pad, pixels), np.float32)
    table[0, : half + 1] = np.cos(angles) * factor
    table[1, : half + 1] = np.sin(angles) * factor
    return table.reshape(2 * pad, pixels)


def tables(count, tile):
    extent = tile + 2 * AMBIT
    inner = folded(count, tile, AMBIT, extent, ROWS)
    wide = folded(count, tile, AMBIT, extent, LANES)
    outer = folded(count, extent, 0, extent, ROWS)
    outer_wide = folded(count, extent, 0, extent, LANES)
    return [
        jnp.asarray(t, jnp.bfloat16)
        for t in (inner, inner.T, wide, wide.T, outer, outer.T, outer_wide, outer_wide.T)
    ]


def quadrants(pupils, weights):
    half = pupils.shape[2] // 2
    scaled = pupils * jnp.sqrt(weights)[None, :, None, None]
    positive_rows = jnp.pad(scaled[:, :, half:], ((0, 0), (0, 0), (0, ROWS - half), (0, 0)))
    negative_rows = jnp.pad(
        jnp.flip(scaled[:, :, :half], 2), ((0, 0), (0, 0), (1, ROWS - half - 1), (0, 0))
    )
    outs = []
    for part in (positive_rows, negative_rows):
        outs.append(jnp.pad(part[..., half:], ((0, 0),) * 3 + ((0, LANES - half),)))
        outs.append(
            jnp.pad(jnp.flip(part[..., :half], 3), ((0, 0),) * 3 + ((1, LANES - half - 1),))
        )
    return outs


def dot(a, b):
    return jnp.dot(a, b, preferred_element_type=jnp.float32)


def times(ar, ai, br, bi):
    return ar * br - ai * bi, ar * bi + ai * br


def work_kernel(
    live_ref, ext_ref, goal_ref, a_ref, b_ref, c_ref, d_ref,
    inner, inner_t, wide, wide_t, outer, outer_t, outer_wide, outer_wide_t,
    total_ref, fields, intensity, slope, spec, acc,
):
    tile = inner.shape[1]
    extent = outer.shape[1]
    kernels = a_ref.shape[1]
    slots = live_ref.shape[1]
    bf = jnp.bfloat16
    total_ref[...] = jnp.zeros_like(total_ref)

    def one_slot(slot, carry):
        base = pl.multiple_of(slot * tile, 128)
        partial_rows = dot(outer[...], ext_ref[:, pl.ds(base, extent)]).astype(bf)
        blocks = dot(partial_rows, outer_wide_t[...])
        cc, cs = blocks[:ROWS, :LANES], blocks[:ROWS, LANES:]
        sc, ss = blocks[ROWS:, :LANES], blocks[ROWS:, LANES:]
        spec[0] = (cc - ss).astype(bf).astype(jnp.float32)
        spec[1] = -((cs + sc).astype(bf).astype(jnp.float32))
        spec[2] = (cc + ss).astype(bf).astype(jnp.float32)
        spec[3] = (cs - sc).astype(bf).astype(jnp.float32)
        intensity[...] = jnp.zeros_like(intensity)
        acc[...] = jnp.zeros_like(acc)

        def forward(k, carry):
            z1r, z1i, z2r, z2i = spec[0], spec[1], spec[2], spec[3]
            ppr, ppi = times(a_ref[0, k], a_ref[1, k], z1r, z1i)
            pnr, pni = times(b_ref[0, k], b_ref[1, k], z2r, z2i)
            npr, npi = times(c_ref[0, k], c_ref[1, k], z2r, -z2i)
            nnr, nni = times(d_ref[0, k], d_ref[1, k], z1r, -z1i)
            pr, pi, mr, mi = ppr + nnr, ppi + nni, ppr - nnr, ppi - nni
            qr, qi, nr, ni = pnr + npr, pni + npi, pnr - npr, pni - npi
            top = jnp.concatenate([pr + qr, ni - mi], axis=1)
            bottom = jnp.concatenate([-(mi + ni), qr - pr], axis=1)
            top_im = jnp.concatenate([pi + qi, mr - nr], axis=1)
            bottom_im = jnp.concatenate([mr + nr, qi - pi], axis=1)
            amplitude = jnp.concatenate([top, bottom, top_im, bottom_im], axis=0).astype(bf)
            section = dot(amplitude, wide[...]).astype(bf)
            section_re, section_im = section[: 2 * ROWS], section[2 * ROWS :]
            step = 128
            for first in range(0, tile, step):
                rows = pl.ds(first, step)
                field_re = dot(inner_t[rows], section_re)
                field_im = dot(inner_t[rows], section_im)
                intensity[rows] += field_re * field_re + field_im * field_im
                fields[k, 0, rows] = field_re.astype(bf)
                fields[k, 1, rows] = field_im.astype(bf)
            return carry

        lax.fori_loop(0, kernels, forward, 0)
        resist = 1.0 / (1.0 + jnp.exp(-steepness * (intensity[...] - threshold_level)))
        live = live_ref[0, slot].astype(jnp.float32)
        goal = goal_ref[:, pl.ds(base, tile)].astype(jnp.float32)
        slope[...] = (
            (2.0 * steepness * live) * (resist - goal) * resist * (1.0 - resist)
        ).astype(bf)

        def backward(k, carry):
            tops = []
            for part in range(2):
                cotangent = slope[...] * fields[k, part]
                columns = dot(cotangent, wide_t[...]).astype(bf)
                tops.append(dot(inner[...], columns))
            re, im = tops
            ccr, csr, scr, ssr = (
                re[:ROWS, :LANES], re[:ROWS, LANES:], re[ROWS:, :LANES], re[ROWS:, LANES:])
            cci, csi, sci, ssi = (
                im[:ROWS, :LANES], im[:ROWS, LANES:], im[ROWS:, :LANES], im[ROWS:, LANES:])
            dr, di, er, ei = ccr - ssr, cci - ssi, ccr + ssr, cci + ssi
            gr, gi, hr, hi = csr + scr, csi + sci, csr - scr, csi - sci
            ppr, ppi = dr + gi, di - gr
            nnr, nni = dr - gi, di + gr
            pnr, pni = er - hi, ei + hr
            npr, npi = er + hi, ei - hr
            ur, ui = times(a_ref[0, k], -a_ref[1, k], ppr, ppi)
            vr, vi = times(d_ref[0, k], d_ref[1, k], nnr, -nni)
            acc[0] += ur + vr
            acc[1] += ui + vi
            ur, ui = times(b_ref[0, k], -b_ref[1, k], pnr, pni)
            vr, vi = times(c_ref[0, k], c_ref[1, k], npr, -npi)
            acc[2] += ur + vr
            acc[3] += ui + vi
            return carry

        lax.fori_loop(0, kernels, backward, 0)
        u1r, u1i, u2r, u2i = acc[0], acc[1], acc[2], acc[3]
        matrix = jnp.concatenate(
            [
                jnp.concatenate([u1r + u2r, u2i - u1i], axis=1),
                jnp.concatenate([-(u1i + u2i), u2r - u1r], axis=1),
            ],
            axis=0,
        ).astype(bf)
        returned = dot(matrix, outer_wide[...]).astype(bf)
        for first in range(0, extent, 128):
            rows = pl.ds(first, 128)
            total_ref[rows, pl.ds(base, extent)] += dot(outer_t[rows], returned)
        return carry

    lax.fori_loop(0, slots, one_slot, 0)


def work(live, extended, goal, quads, consts):
    tile = goal.shape[0]
    kernels = quads[0].shape[1]
    vmem = pl.BlockSpec(memory_space=pltpu.VMEM)
    return pl.pallas_call(
        work_kernel,
        out_shape=jax.ShapeDtypeStruct(extended.shape, jnp.float32),
        in_specs=[pl.BlockSpec(memory_space=pltpu.SMEM)] + [vmem] * 14,
        out_specs=vmem,
        scratch_shapes=[
            pltpu.VMEM((kernels, 2, tile, tile), jnp.bfloat16),
            pltpu.VMEM((tile, tile), jnp.float32),
            pltpu.VMEM((tile, tile), jnp.bfloat16),
            pltpu.VMEM((4, ROWS, LANES), jnp.float32),
            pltpu.VMEM((4, ROWS, LANES), jnp.float32),
        ],
        cost_estimate=pl.CostEstimate(
            flops=20_000_000_000, bytes_accessed=16_000_000, transcendentals=524288
        ),
        compiler_params=pltpu.CompilerParams(vmem_limit_bytes=60 * 1024 * 1024),
    )(live, extended, goal, *quads, *consts)


def extended_2(block, sides, width):
    for axis, dim in sides:
        count = lax.axis_size(axis)
        forward = [(i, i + 1) for i in range(count - 1)]
        backward = [(target, source) for source, target in forward]
        low = lax.ppermute(
            lax.slice_in_dim(block, block.shape[dim] - width, None, axis=dim), axis, forward
        )
        high = lax.ppermute(lax.slice_in_dim(block, 0, width, axis=dim), axis, backward)
        block = jnp.concatenate([low, block, high], axis=dim)
    return block


def fold_rims(total, tile_size, block_width, ambit_size):
    beside_all = extended_2(
        total.astype(jnp.bfloat16), (("row", 0), ("col", 1)), ambit_size
    ).astype(total.dtype)
    middle_rows = beside_all[2 * ambit_size : 2 * ambit_size + tile_size]
    middle_rows = middle_rows.at[:ambit_size].add(beside_all[:ambit_size])
    middle_rows = middle_rows.at[tile_size - ambit_size :].add(
        beside_all[tile_size + 3 * ambit_size :]
    )
    folded = middle_rows[:, 2 * ambit_size : 2 * ambit_size + block_width]
    folded = folded.at[:, :ambit_size].add(middle_rows[:, :ambit_size])
    folded = folded.at[:, block_width - ambit_size :].add(
        middle_rows[:, block_width + 3 * ambit_size :]
    )
    return folded


def body(mask, target, live, pupils, weights):
    tile = mask.shape[0]
    consts = tables(pupils.shape[2], tile)
    quads = quadrants(pupils, weights)
    extended = extended_2(mask.astype(jnp.bfloat16), (("row", 0), ("col", 1)), AMBIT)
    total = work(live, extended, target, quads, consts)
    folded = fold_rims(total, tile, mask.shape[1], AMBIT)
    return mask - step_rate * folded


def solution(mesh):
    return jax.shard_map(
        body,
        mesh=mesh,
        in_specs=(P("row", "col"), P("row", "col"), P("row", "col"), P(), P()),
        out_specs=P("row", "col"),
        check_vma=False,
    )
```

```python
from functools import partial
import math

import jax
import jax.numpy as jnp
import numpy as np
from jax import lax
from jax.experimental import pallas as pl
from jax.experimental.pallas import tpu as pltpu
from jax.sharding import PartitionSpec as P

AMBIT = 128
ROWS = 80
LANES = 128

steepness = 4.0
threshold_level = 1.0
step_rate = 8.0


def folded(count, pixels, offset, period, pad):
    half = count // 2
    frequency = np.arange(half + 1)
    place = np.arange(pixels) + offset
    phases = np.mod(frequency[:, None] * place[None, :], period).astype(np.float32)
    angles = phases * np.float32(2.0 * math.pi / period)
    factor = np.float32(1.0 / math.sqrt(period))
    table = np.zeros((2, pad, pixels), np.float32)
    table[0, : half + 1] = np.cos(angles) * factor
    table[1, : half + 1] = np.sin(angles) * factor
    return table.reshape(2 * pad, pixels)


def tables(count, tile):
    extent = tile + 2 * AMBIT
    inner = folded(count, tile, AMBIT, extent, ROWS)
    wide = folded(count, tile, AMBIT, extent, LANES)
    outer = folded(count, extent, 0, extent, ROWS)
    outer_wide = folded(count, extent, 0, extent, LANES)
    half = count // 2
    left = np.zeros((2 * ROWS, count), np.float32)
    right = np.zeros((2 * LANES, count), np.float32)
    for table, pad in ((left, ROWS), (right, LANES)):
        for f in range(half + 1):
            if f < half:
                table[f, half + f] = 1.0
            if f > 0:
                table[pad + f, half - f] = 1.0
    return [
        jnp.asarray(t, jnp.bfloat16)
        for t in (
            inner, inner.T, wide, wide.T, outer, outer.T, outer_wide, outer_wide.T, left, right.T,
        )
    ]


def dot(a, b):
    return jnp.dot(a, b, preferred_element_type=jnp.float32)


def times(ar, ai, br, bi):
    return ar * br - ai * bi, ar * bi + ai * br


def quarter(ref, part, k):
    return (
        ref[part, k, :ROWS, :LANES],
        ref[part, k, :ROWS, LANES:],
        ref[part, k, ROWS:, :LANES],
        ref[part, k, ROWS:, LANES:],
    )


def fold_pupils(pupils, weights, left, right, quads):
    bf = jnp.bfloat16

    def one(k, carry):
        root = jnp.sqrt(jnp.full((1, pupils.shape[3]), weights[k], jnp.float32))
        for part in range(2):
            value = pupils[part, k] * root
            high = value.astype(bf)
            low = (value - high.astype(jnp.float32)).astype(bf)
            moved = [dot(left[...], dot(v, right[...]).astype(bf)) for v in (high, low)]
            quads[part, k] = moved[0] + moved[1]
        return carry

    lax.fori_loop(0, pupils.shape[1], one, 0)


def take_spectrum(window, outer, outer_wide_t, spec):
    bf = jnp.bfloat16
    partial_rows = dot(outer[...], window).astype(bf)
    blocks = dot(partial_rows, outer_wide_t[...])
    cc, cs = blocks[:ROWS, :LANES], blocks[:ROWS, LANES:]
    sc, ss = blocks[ROWS:, :LANES], blocks[ROWS:, LANES:]
    spec[0] = (cc - ss).astype(bf).astype(jnp.float32)
    spec[1] = -((cs + sc).astype(bf).astype(jnp.float32))
    spec[2] = (cc + ss).astype(bf).astype(jnp.float32)
    spec[3] = (cs - sc).astype(bf).astype(jnp.float32)


def amplitude_of(k, quads, spec):
    ar, br, cr, dr = quarter(quads, 0, k)
    ai, bi, ci, di = quarter(quads, 1, k)
    z1r, z1i, z2r, z2i = spec[0], spec[1], spec[2], spec[3]
    ppr, ppi = times(ar, ai, z1r, z1i)
    pnr, pni = times(br, bi, z2r, z2i)
    npr, npi = times(cr, ci, z2r, -z2i)
    nnr, nni = times(dr, di, z1r, -z1i)
    pr, pi, mr, mi = ppr + nnr, ppi + nni, ppr - nnr, ppi - nni
    qr, qi, nr, ni = pnr + npr, pni + npi, pnr - npr, pni - npi
    return jnp.concatenate(
        [
            jnp.concatenate([pr + qr, ni - mi], axis=1),
            jnp.concatenate([-(mi + ni), qr - pr], axis=1),
            jnp.concatenate([pi + qi, mr - nr], axis=1),
            jnp.concatenate([mr + nr, qi - pi], axis=1),
        ],
        axis=0,
    ).astype(jnp.bfloat16)


def gather_adjoint(k, re, im, quads, acc):
    ar, br, cr, dr = quarter(quads, 0, k)
    ai, bi, ci, di = quarter(quads, 1, k)
    ccr, csr, scr, ssr = re[:ROWS, :LANES], re[:ROWS, LANES:], re[ROWS:, :LANES], re[ROWS:, LANES:]
    cci, csi, sci, ssi = im[:ROWS, :LANES], im[:ROWS, LANES:], im[ROWS:, :LANES], im[ROWS:, LANES:]
    er, ei, fr, fi = ccr - ssr, cci - ssi, ccr + ssr, cci + ssi
    gr, gi, hr, hi = csr + scr, csi + sci, csr - scr, csi - sci
    ur, ui = times(ar, -ai, er + gi, ei - gr)
    vr, vi = times(dr, di, er - gi, -(ei + gr))
    acc[0] += ur + vr
    acc[1] += ui + vi
    ur, ui = times(br, -bi, fr - hi, fi + hr)
    vr, vi = times(cr, ci, fr + hi, hr - fi)
    acc[2] += ur + vr
    acc[3] += ui + vi


def spectral_matrix(acc):
    u1r, u1i, u2r, u2i = acc[0], acc[1], acc[2], acc[3]
    return jnp.concatenate(
        [
            jnp.concatenate([u1r + u2r, u2i - u1i], axis=1),
            jnp.concatenate([-(u1i + u2i), u2r - u1r], axis=1),
        ],
        axis=0,
    ).astype(jnp.bfloat16)


def pieces(tile, width):
    low, high = tile + AMBIT, width + AMBIT
    split = tile + 2 * AMBIT
    rows = {-1: ((AMBIT, AMBIT), low), 0: ((AMBIT, tile), AMBIT), 1: ((tile, AMBIT), 0)}
    outs = []
    for slot in range(2):
        for dr in (-1, 1, 0):
            (first, count), place = rows[dr]
            if dr:
                c0, c1 = ((AMBIT, split), (split, high))[slot]
                outs.append((slot, dr, 0, (first, count, c0, c1 - c0), (place, count, c0, c1 - c0)))
            if slot == 0:
                outs.append((0, dr, 1, (first, count, width, AMBIT), (place, count, 0, AMBIT)))
            else:
                outs.append((1, dr, -1, (first, count, AMBIT, AMBIT), (place, count, high, AMBIT)))
    return outs


def rims(tile, width):
    low, high = tile + AMBIT, width + AMBIT
    cut = tile - AMBIT
    outs = []
    for slot in range(2):
        for dr in (-1, 1, 0):
            first, count = ((AMBIT, tile), (low, AMBIT), (0, AMBIT))[dr]
            side = 1 if dr < 0 else 0
            if dr:
                c0, c1 = ((AMBIT, tile), (tile, high))[slot]
                outs.append((slot, dr, 0, (first, count, c0, c1 - c0), ("rows", side, c0 - AMBIT, c1 - c0)))
            dc, c0, other = ((-1, 0, 1), (1, high, 0))[slot]
            if dr:
                outs.append((slot, dr, dc, (first, count, c0, AMBIT), ("corner", 2 * side + other)))
            else:
                outs.append((slot, 0, dc, (first, count, c0, AMBIT), ("cols", other)))
    return outs


def window(ref, place):
    row, rows, col, cols = place
    return ref.at[pl.ds(row, rows), pl.ds(col, cols)]


def kernel(
    grid, live_ref, weight_ref, mask_hbm, goal_hbm, pupil_hbm, *refs,
):
    tables_hbm, refs = refs[:10], refs[10:]
    out_hbm = refs[0]
    held, refs = refs[1:11], refs[11:]
    (
        mask, goal, pupils, quads, ext, total, fields, intensity, slope, spec, acc, section,
        rim, got_rows, got_cols, got_corner, in_sem, halo_send, halo_recv, rim_send, rim_recv, out_sem,
    ) = refs
    inner, inner_t, wide, wide_t, outer, outer_t, outer_wide, outer_wide_t, left, right = held
    bf = jnp.bfloat16
    tile, width = mask.shape
    extent = tile + 2 * AMBIT
    kernels = pupils.shape[1]
    row, col = lax.axis_index("row"), lax.axis_index("col")
    last_row, last_col = grid[0] - 1, grid[1] - 1

    def there(dr, dc):
        ok = jnp.bool_(True)
        if dr:
            ok = row > 0 if dr < 0 else row < last_row
        if dc:
            side = col > 0 if dc < 0 else col < last_col
            ok = jnp.logical_and(ok, side) if dr else side
        return ok

    def only(dr, dc, act):
        pl.when(there(dr, dc))(act)

    cuts = ((0, AMBIT), (tile - AMBIT, AMBIT), (AMBIT, tile - 2 * AMBIT))
    loads = [
        pltpu.make_async_copy(mask_hbm.at[pl.ds(a, n)], mask.at[pl.ds(a, n)], in_sem.at[i])
        for i, (a, n) in enumerate(cuts)
    ]
    loads.append(pltpu.make_async_copy(pupil_hbm, pupils, in_sem.at[3]))
    order = (8, 9, 4, 7, 2, 1, 3, 0, 6, 5)
    at = {}
    for t in order:
        at[t] = len(loads)
        loads.append(pltpu.make_async_copy(tables_hbm[t], held[t], in_sem.at[len(loads)]))
    goal_load = len(loads)
    loads.append(pltpu.make_async_copy(goal_hbm, goal, in_sem.at[goal_load]))
    for load in loads:
        load.start()

    barrier = pltpu.get_barrier_semaphore()
    around = [(dr, dc) for dr in (-1, 0, 1) for dc in (-1, 0, 1) if dr or dc]
    for dr, dc in around:
        only(dr, dc, lambda: pl.semaphore_signal(
            barrier, inc=1, device_id=(row + dr, col + dc), device_id_type=pl.DeviceIdType.MESH))
    for i, (a, n) in enumerate(cuts):
        loads[i].wait()
        ext[pl.ds(AMBIT + a, n), pl.ds(AMBIT, width)] = mask[pl.ds(a, n)].astype(bf)
    tall = 3 - (row == 0).astype(jnp.int32) - (row == last_row).astype(jnp.int32)
    broad = 3 - (col == 0).astype(jnp.int32) - (col == last_col).astype(jnp.int32)
    pl.semaphore_wait(barrier, tall * broad - 1)

    def copies(table, source, target, send, recv):
        outs = []
        for i, (slot, dr, dc, src, dst) in enumerate(table):
            outs.append((slot, dr, dc, pltpu.make_async_remote_copy(
                src_ref=window(source, src), dst_ref=target(dst), send_sem=send.at[i],
                recv_sem=recv.at[i], device_id=(row + dr, col + dc),
                device_id_type=pl.DeviceIdType.MESH)))
        return outs

    def place(dst):
        if dst[0] == "rows":
            return got_rows.at[dst[1], :, pl.ds(dst[2], dst[3])]
        return got_cols.at[dst[1]] if dst[0] == "cols" else got_corner.at[dst[1]]

    halo = copies(pieces(tile, width), ext, lambda dst: window(ext, dst), halo_send, halo_recv)
    back = copies(rims(tile, width), rim, place, rim_send, rim_recv)
    for slot, dr, dc, copy in halo:
        only(dr, dc, copy.start)
    for slot, dr, dc, src, dst in pieces(tile, width):

        def clear():
            ext[pl.ds(dst[0], dst[1]), pl.ds(dst[2], dst[3])] = jnp.zeros((dst[1], dst[3]), bf)

        pl.when(jnp.logical_not(there(-dr, -dc)))(clear)

    loads[3].wait()
    for t in order[:2]:
        loads[at[t]].wait()
    fold_pupils(pupils, weight_ref, left, right, quads)
    for t in order[2:]:
        loads[at[t]].wait()
    loads[goal_load].wait()

    for now in range(2):
        for slot, dr, dc, copy in halo:
            if slot == now:
                only(-dr, -dc, copy.wait_recv)
        base = now * tile
        take_spectrum(ext[:, pl.ds(base, extent)], outer, outer_wide_t, spec)
        intensity[...] = jnp.zeros_like(intensity)
        acc[...] = jnp.zeros_like(acc)

        def forward(k, carry):
            amplitude = amplitude_of(k, quads, spec)
            section = dot(amplitude, wide[...]).astype(bf)
            section_re, section_im = section[: 2 * ROWS], section[2 * ROWS :]
            step = 128
            for first in range(0, tile, step):
                rows = pl.ds(first, step)
                field_re = dot(inner_t[rows], section_re)
                field_im = dot(inner_t[rows], section_im)
                intensity[rows] += field_re * field_re + field_im * field_im
                fields[k, 0, rows] = field_re.astype(bf)
                fields[k, 1, rows] = field_im.astype(bf)
            return carry

        lax.fori_loop(0, kernels, forward, 0)
        resist = 1.0 / (1.0 + jnp.exp(-steepness * (intensity[...] - threshold_level)))
        live = live_ref[0, now].astype(jnp.float32)
        wanted = goal[:, pl.ds(base, tile)].astype(jnp.float32)
        slope[...] = (
            (2.0 * steepness * live) * (resist - wanted) * resist * (1.0 - resist)
        ).astype(bf)

        def backward(k, carry):
            tops = []
            for part in range(2):
                columns = dot(slope[...] * fields[k, part], wide_t[...]).astype(bf)
                tops.append(dot(inner[...], columns))
            gather_adjoint(k, *tops, quads, acc)
            return carry

        lax.fori_loop(0, kernels, backward, 0)
        returned = dot(spectral_matrix(acc), outer_wide[...]).astype(bf)
        for first in (0, tile + AMBIT) + tuple(range(AMBIT, tile + AMBIT, AMBIT)):
            rows = pl.ds(first, AMBIT)
            piece = dot(outer_t[rows], returned)
            edge = first in (0, tile + AMBIT)
            if now == 0:
                total[rows, pl.ds(0, extent)] = piece
                final = piece[:, :tile]
                if edge:
                    rim[rows, pl.ds(0, tile)] = final.astype(bf)
                else:
                    rim[rows, pl.ds(0, AMBIT)] = final[:, :AMBIT].astype(bf)
            else:
                both = total[rows, pl.ds(tile, extent - tile)] + piece[:, : extent - tile]
                total[rows, pl.ds(tile, extent - tile)] = both
                total[rows, pl.ds(extent, tile)] = piece[:, extent - tile :]
                if edge:
                    rim[rows, pl.ds(tile, extent - tile)] = both.astype(bf)
                    rim[rows, pl.ds(extent, tile)] = piece[:, extent - tile :].astype(bf)
                else:
                    rim[rows, pl.ds(width + AMBIT, AMBIT)] = piece[:, tile + AMBIT :].astype(bf)
        for slot, dr, dc, copy in back:
            if slot == now:
                only(dr, dc, copy.start)

    mask[...] = mask[...] - step_rate * total[pl.ds(AMBIT, tile), pl.ds(AMBIT, width)]
    inside = (AMBIT, tile - 2 * AMBIT, AMBIT, width - 2 * AMBIT)

    def put(place, sem):
        return pltpu.make_async_copy(window(mask, place), window(out_hbm, place), out_sem.at[sem])

    areas = (
        inside,
        (0, AMBIT, 0, width),
        (tile - AMBIT, AMBIT, 0, width),
        (AMBIT, tile - 2 * AMBIT, 0, AMBIT),
        (AMBIT, tile - 2 * AMBIT, width - AMBIT, AMBIT),
    )
    puts = [put(a, i) for i, a in enumerate(areas)]
    puts[0].start()
    for now in range(2):
        for (slot, dr, dc, copy), entry in zip(back, rims(tile, width)):
            if slot != now:
                continue
            dst = entry[4]

            def add():
                copy.wait_recv()
                if dst[0] == "rows":
                    spot = (dst[1] * (tile - AMBIT), AMBIT, dst[2], dst[3])
                elif dst[0] == "cols":
                    spot = (0, tile, dst[1] * (width - AMBIT), AMBIT)
                else:
                    spot = (
                        dst[1] // 2 * (tile - AMBIT), AMBIT, dst[1] % 2 * (width - AMBIT), AMBIT)
                r, n, c, m = spot
                mask[pl.ds(r, n), pl.ds(c, m)] -= step_rate * place(dst)[...].astype(jnp.float32)

            only(-dr, -dc, add)
    for p in puts[1:]:
        p.start()
    for p in puts:
        p.wait()
    for slot, dr, dc, copy in halo + back:
        only(dr, dc, copy.wait_send)


def body(grid, mask, target, live, pupils, weights):
    tile, width = mask.shape
    consts = tables(pupils.shape[2], tile)
    kernels = pupils.shape[1]
    bf, f32 = jnp.bfloat16, jnp.float32
    anywhere = pl.BlockSpec(memory_space=pl.ANY)
    smem = pl.BlockSpec(memory_space=pltpu.SMEM)
    extent = tile + 2 * AMBIT
    return pl.pallas_call(
        partial(kernel, grid),
        out_shape=jax.ShapeDtypeStruct(mask.shape, f32),
        in_specs=[smem, smem] + [anywhere] * 13,
        out_specs=anywhere,
        scratch_shapes=[pltpu.VMEM(t.shape, t.dtype) for t in consts]
        + [
            pltpu.VMEM((tile, width), f32),
            pltpu.VMEM((tile, width), bf),
            pltpu.VMEM(pupils.shape, f32),
            pltpu.VMEM((2, kernels, 2 * ROWS, 2 * LANES), f32),
            pltpu.VMEM((extent, width + 2 * AMBIT), bf),
            pltpu.VMEM((extent, width + 2 * AMBIT), f32),
            pltpu.VMEM((kernels, 2, tile, tile), bf),
            pltpu.VMEM((tile, tile), f32),
            pltpu.VMEM((tile, tile), bf),
            pltpu.VMEM((4, ROWS, LANES), f32),
            pltpu.VMEM((4, ROWS, LANES), f32),
            pltpu.VMEM((2, 4 * ROWS, tile), bf),
            pltpu.VMEM((extent, width + 2 * AMBIT), bf),
            pltpu.VMEM((2, AMBIT, width), bf),
            pltpu.VMEM((2, tile, AMBIT), bf),
            pltpu.VMEM((4, AMBIT, AMBIT), bf),
            pltpu.SemaphoreType.DMA((15,)),
            pltpu.SemaphoreType.DMA((10,)),
            pltpu.SemaphoreType.DMA((10,)),
            pltpu.SemaphoreType.DMA((10,)),
            pltpu.SemaphoreType.DMA((10,)),
            pltpu.SemaphoreType.DMA((5,)),
        ],
        compiler_params=pltpu.CompilerParams(
            collective_id=0, has_side_effects=True, vmem_limit_bytes=60 * 1024 * 1024
        ),
    )(live, weights, mask, target, pupils, *consts)


def solution(mesh):
    return jax.shard_map(
        partial(body, (mesh.shape["row"], mesh.shape["col"])),
        mesh=mesh,
        in_specs=(P("row", "col"), P("row", "col"), P("row", "col"), P(), P()),
        out_specs=P("row", "col"),
        check_vma=False,
    )
```

```python
from functools import partial
import math

import jax
import jax.numpy as jnp
import numpy as np
from jax import lax
from jax.experimental import pallas as pl
from jax.experimental.pallas import tpu as pltpu
from jax.sharding import PartitionSpec as P

AMBIT = 128
ROWS = 80
LANES = 128

steepness = 4.0
threshold_level = 1.0
step_rate = 8.0

UNROLL = 1
VMEM_LIMIT = 60 * 1024 * 1024


def folded(count, pixels, offset, period, pad):
    half = count // 2
    frequency = np.arange(half + 1)
    place = np.arange(pixels) + offset
    phases = np.mod(frequency[:, None] * place[None, :], period).astype(np.float32)
    angles = phases * np.float32(2.0 * math.pi / period)
    factor = np.float32(1.0 / math.sqrt(period))
    table = np.zeros((2, pad, pixels), np.float32)
    table[0, : half + 1] = np.cos(angles) * factor
    table[1, : half + 1] = np.sin(angles) * factor
    return table.reshape(2 * pad, pixels)


def grid_table(count, points, period, pad):
    half = count // 2
    angles = np.arange(half + 1)[:, None] * np.arange(points)[None, :] * (2.0 * math.pi / points)
    table = np.zeros((2, pad, points))
    table[0, : half + 1] = np.cos(angles) / math.sqrt(period)
    table[1, : half + 1] = np.sin(angles) / math.sqrt(period)
    return table.reshape(2 * pad, points)


def between(count, points, pixels, offset, period):
    gap = np.arange(pixels)[:, None] + offset - np.arange(points)[None, :] * (period / points)
    gap = gap * (2.0 * math.pi / period)
    return (1.0 + 2.0 * sum(np.cos(m * gap) for m in range(1, count + 1))) / points


def halves(table):
    high = table.astype(jnp.bfloat16).astype(np.float64)
    return high, table - high


def tables(count, tile):
    extent = tile + 2 * AMBIT
    rows = -(-(2 * count + 1) // 16) * 16
    lanes = -(-(2 * count + 1) // 128) * 128
    grid_rows = grid_table(count, rows, extent, ROWS)
    grid_lanes = grid_table(count, lanes, extent, LANES)
    over_rows = between(count, rows, tile, AMBIT, extent)
    over_lanes = between(count, lanes, tile, AMBIT, extent)
    outer_wide = folded(count, extent, 0, extent, LANES)
    half = count // 2
    left = np.zeros((2 * ROWS, count), np.float32)
    right = np.zeros((2 * LANES, count), np.float32)
    for table, pad in ((left, ROWS), (right, LANES)):
        for f in range(half + 1):
            if f < half:
                table[f, half + f] = 1.0
            if f > 0:
                table[pad + f, half - f] = 1.0
    rows_high, rows_low = halves(over_rows)
    lanes_high, lanes_low = halves(over_lanes.T)
    return [
        jnp.asarray(t, jnp.bfloat16)
        for t in (
            left, right.T, outer_wide, grid_lanes, grid_rows.T, rows_high, rows_low, lanes_high,
            lanes_low, rows_high.T, grid_rows,
        )
    ]


def dot(a, b):
    return jnp.dot(a, b, preferred_element_type=jnp.float32)


def split(value):
    upper = value.astype(jnp.bfloat16)
    return upper, (value - upper.astype(jnp.float32)).astype(jnp.bfloat16)


def times(ar, ai, br, bi):
    return ar * br - ai * bi, ar * bi + ai * br


def quarter(ref, part, k):
    return (
        ref[part, k, :ROWS, :LANES],
        ref[part, k, :ROWS, LANES:],
        ref[part, k, ROWS:, :LANES],
        ref[part, k, ROWS:, LANES:],
    )


def fold_pupils(pupils, weights, left, right, quads):
    bf = jnp.bfloat16

    def one(k, carry):
        root = jnp.sqrt(jnp.full((1, pupils.shape[3]), weights[k], jnp.float32))
        for part in range(2):
            value = pupils[part, k] * root
            moved = [dot(left[...], dot(v, right[...]).astype(bf)) for v in split(value)]
            quads[part, k] = moved[0] + moved[1]
        return carry

    lax.fori_loop(0, pupils.shape[1], one, 0)


def take_spectrum(window, outer_wide, outer_wide_t, spec):
    bf = jnp.bfloat16
    folds = jnp.concatenate([outer_wide[:ROWS], outer_wide[LANES : LANES + ROWS]], axis=0)
    partial_rows = dot(folds, window).astype(bf)
    blocks = dot(partial_rows, outer_wide_t[...])
    cc, cs = blocks[:ROWS, :LANES], blocks[:ROWS, LANES:]
    sc, ss = blocks[ROWS:, :LANES], blocks[ROWS:, LANES:]
    spec[0] = (cc - ss).astype(bf).astype(jnp.float32)
    spec[1] = -((cs + sc).astype(bf).astype(jnp.float32))
    spec[2] = (cc + ss).astype(bf).astype(jnp.float32)
    spec[3] = (cs - sc).astype(bf).astype(jnp.float32)


def amplitude_of(k, quads, spec):
    ar, br, cr, dr = quarter(quads, 0, k)
    ai, bi, ci, di = quarter(quads, 1, k)
    z1r, z1i, z2r, z2i = spec[0], spec[1], spec[2], spec[3]
    ppr, ppi = times(ar, ai, z1r, z1i)
    pnr, pni = times(br, bi, z2r, z2i)
    npr, npi = times(cr, ci, z2r, -z2i)
    nnr, nni = times(dr, di, z1r, -z1i)
    pr, pi, mr, mi = ppr + nnr, ppi + nni, ppr - nnr, ppi - nni
    qr, qi, nr, ni = pnr + npr, pni + npi, pnr - npr, pni - npi
    return jnp.concatenate(
        [
            jnp.concatenate([pr + qr, ni - mi], axis=1),
            jnp.concatenate([-(mi + ni), qr - pr], axis=1),
            jnp.concatenate([pi + qi, mr - nr], axis=1),
            jnp.concatenate([mr + nr, qi - pi], axis=1),
        ],
        axis=0,
    ).astype(jnp.bfloat16)


def gather_adjoint(k, re, im, quads, acc):
    ar, br, cr, dr = quarter(quads, 0, k)
    ai, bi, ci, di = quarter(quads, 1, k)
    ccr, csr, scr, ssr = re[:ROWS, :LANES], re[:ROWS, LANES:], re[ROWS:, :LANES], re[ROWS:, LANES:]
    cci, csi, sci, ssi = im[:ROWS, :LANES], im[:ROWS, LANES:], im[ROWS:, :LANES], im[ROWS:, LANES:]
    er, ei, fr, fi = ccr - ssr, cci - ssi, ccr + ssr, cci + ssi
    gr, gi, hr, hi = csr + scr, csi + sci, csr - scr, csi - sci
    ur, ui = times(ar, -ai, er + gi, ei - gr)
    vr, vi = times(dr, di, er - gi, -(ei + gr))
    acc[0] += ur + vr
    acc[1] += ui + vi
    ur, ui = times(br, -bi, fr - hi, fi + hr)
    vr, vi = times(cr, ci, fr + hi, hr - fi)
    acc[2] += ur + vr
    acc[3] += ui + vi


def spectral_matrix(acc):
    u1r, u1i, u2r, u2i = acc[0], acc[1], acc[2], acc[3]
    rest = jnp.zeros((LANES - ROWS, 2 * LANES), jnp.float32)
    return jnp.concatenate(
        [
            jnp.concatenate([u1r + u2r, u2i - u1i], axis=1),
            rest,
            jnp.concatenate([-(u1i + u2i), u2r - u1r], axis=1),
            rest,
        ],
        axis=0,
    ).astype(jnp.bfloat16)


def pieces(tile, width):
    low, high = tile + AMBIT, width + AMBIT
    split = tile + 2 * AMBIT
    rows = {-1: ((AMBIT, AMBIT), low), 0: ((AMBIT, tile), AMBIT), 1: ((tile, AMBIT), 0)}
    outs = []
    for slot in range(2):
        for dr in (-1, 1, 0):
            (first, count), place = rows[dr]
            if dr:
                c0, c1 = ((AMBIT, split), (split, high))[slot]
                outs.append((slot, dr, 0, (first, count, c0, c1 - c0), (place, count, c0, c1 - c0)))
            if slot == 0:
                outs.append((0, dr, 1, (first, count, width, AMBIT), (place, count, 0, AMBIT)))
            else:
                outs.append((1, dr, -1, (first, count, AMBIT, AMBIT), (place, count, high, AMBIT)))
    return outs


def rims(tile, width):
    low, high = tile + AMBIT, width + AMBIT
    cut = tile - AMBIT
    outs = []
    for slot in range(2):
        for dr in (-1, 1, 0):
            first, count = ((AMBIT, tile), (low, AMBIT), (0, AMBIT))[dr]
            side = 1 if dr < 0 else 0
            if dr:
                c0, c1 = ((AMBIT, tile), (tile, high))[slot]
                outs.append((slot, dr, 0, (first, count, c0, c1 - c0), ("rows", side, c0 - AMBIT, c1 - c0)))
            dc, c0, other = ((-1, 0, 1), (1, high, 0))[slot]
            if dr:
                outs.append((slot, dr, dc, (first, count, c0, AMBIT), ("corner", 2 * side + other)))
            else:
                outs.append((slot, 0, dc, (first, count, c0, AMBIT), ("cols", other)))
    return outs


def window(ref, place):
    row, rows, col, cols = place
    return ref.at[pl.ds(row, rows), pl.ds(col, cols)]


def kernel(
    grid, live_ref, weight_ref, mask_hbm, goal_hbm, pupil_hbm, *refs,
):
    tables_hbm, refs = refs[:11], refs[11:]
    out = refs[0]
    held, refs = refs[1:12], refs[12:]
    (
        mask, goal, pupils, quads, ext, total, fields, intensity, slope, sloped, spec, acc,
        outer_wide_t, grid_lanes_t, over_lanes, high, low, rim, got_rows, got_cols, got_corner, in_sem, halo_send, halo_recv, rim_send, rim_recv,
    ) = refs
    (
        left, right, outer_wide, grid_lanes, grid_rows_t, rows_high, rows_low, lanes_high,
        lanes_low, over_rows_t, grid_rows,
    ) = held
    bf = jnp.bfloat16
    tile, width = mask.shape
    extent = tile + 2 * AMBIT
    kernels = pupils.shape[1]
    row, col = lax.axis_index("row"), lax.axis_index("col")
    last_row, last_col = grid[0] - 1, grid[1] - 1

    def there(dr, dc):
        ok = jnp.bool_(True)
        if dr:
            ok = row > 0 if dr < 0 else row < last_row
        if dc:
            side = col > 0 if dc < 0 else col < last_col
            ok = jnp.logical_and(ok, side) if dr else side
        return ok

    def only(dr, dc, act):
        pl.when(there(dr, dc))(act)

    cuts = ((0, AMBIT), (tile - AMBIT, AMBIT), (AMBIT, tile - 2 * AMBIT))
    loads = [
        pltpu.make_async_copy(mask_hbm.at[pl.ds(a, n)], mask.at[pl.ds(a, n)], in_sem.at[i])
        for i, (a, n) in enumerate(cuts)
    ]
    loads.append(pltpu.make_async_copy(pupil_hbm, pupils, in_sem.at[3]))
    first_table = len(loads)
    for source, target in zip(tables_hbm, held):
        loads.append(pltpu.make_async_copy(source, target, in_sem.at[len(loads)]))
    goal_load = len(loads)
    loads.append(pltpu.make_async_copy(goal_hbm, goal, in_sem.at[goal_load]))
    for load in loads:
        load.start()

    barrier = pltpu.get_barrier_semaphore()
    around = [(dr, dc) for dr in (-1, 0, 1) for dc in (-1, 0, 1) if dr or dc]
    for dr, dc in around:
        only(dr, dc, lambda: pl.semaphore_signal(
            barrier, inc=1, device_id=(row + dr, col + dc), device_id_type=pl.DeviceIdType.MESH))
    for i, (a, n) in enumerate(cuts):
        loads[i].wait()
        ext[pl.ds(AMBIT + a, n), pl.ds(AMBIT, width)] = mask[pl.ds(a, n)].astype(bf)
    tall = 3 - (row == 0).astype(jnp.int32) - (row == last_row).astype(jnp.int32)
    broad = 3 - (col == 0).astype(jnp.int32) - (col == last_col).astype(jnp.int32)
    pl.semaphore_wait(barrier, tall * broad - 1)

    def copies(table, source, target, send, recv):
        outs = []
        for i, (slot, dr, dc, src, dst) in enumerate(table):
            outs.append((slot, dr, dc, pltpu.make_async_remote_copy(
                src_ref=window(source, src), dst_ref=target(dst), send_sem=send.at[i],
                recv_sem=recv.at[i], device_id=(row + dr, col + dc),
                device_id_type=pl.DeviceIdType.MESH)))
        return outs

    def place(dst):
        if dst[0] == "rows":
            return got_rows.at[dst[1], :, pl.ds(dst[2], dst[3])]
        return got_cols.at[dst[1]] if dst[0] == "cols" else got_corner.at[dst[1]]

    halo = copies(pieces(tile, width), ext, lambda dst: window(ext, dst), halo_send, halo_recv)
    back = copies(rims(tile, width), rim, place, rim_send, rim_recv)
    for slot, dr, dc, copy in halo:
        only(dr, dc, copy.start)
    for slot, dr, dc, src, dst in pieces(tile, width):

        def clear():
            ext[pl.ds(dst[0], dst[1]), pl.ds(dst[2], dst[3])] = jnp.zeros((dst[1], dst[3]), bf)

        pl.when(jnp.logical_not(there(-dr, -dc)))(clear)

    loads[3].wait()
    for load in loads[first_table : first_table + 2]:
        load.wait()
    fold_pupils(pupils, weight_ref, left, right, quads)
    for load in loads[first_table + 2 :]:
        load.wait()
    points = grid_rows.shape[1]
    outer_wide_t[...] = outer_wide[...].T
    grid_lanes_t[...] = grid_lanes[...].T
    over_lanes[...] = lanes_high[...].T

    for now in range(2):
        for slot, dr, dc, copy in halo:
            if slot == now:
                only(-dr, -dc, copy.wait_recv)
        base = now * tile
        take_spectrum(ext[:, pl.ds(base, extent)], outer_wide, outer_wide_t, spec)
        intensity[...] = jnp.zeros_like(intensity)
        acc[...] = jnp.zeros_like(acc)

        def forward(k, carry):
            section = dot(amplitude_of(k, quads, spec), grid_lanes[...]).astype(bf)
            field_re = dot(grid_rows_t[...], section[: 2 * ROWS])
            field_im = dot(grid_rows_t[...], section[2 * ROWS :])
            intensity[...] += field_re * field_re + field_im * field_im
            fields[k, :points] = field_re.astype(bf)
            fields[k, points:] = field_im.astype(bf)
            return carry

        lax.fori_loop(0, kernels, forward, 0, unroll=UNROLL)
        high[...], low[...] = split(intensity[...])
        live = live_ref[0, now].astype(jnp.float32)
        for first in range(0, tile, 128):
            rows = pl.ds(first, 128)
            level = dot(rows_high[rows], high[...]) + dot(rows_high[rows], low[...])
            level = level + dot(rows_low[rows], high[...])
            upper, lower = split(level)
            level = dot(upper, lanes_high[...]) + dot(lower, lanes_high[...])
            level = level + dot(upper, lanes_low[...])
            resist = 1.0 / (1.0 + jnp.exp(-steepness * (level - threshold_level)))
            wanted = goal[rows, pl.ds(base, tile)].astype(jnp.float32)
            slope[rows] = (
                (2.0 * steepness * live) * (resist - wanted) * resist * (1.0 - resist)
            ).astype(bf)
        sloped[...] = dot(dot(over_rows_t[...], slope[...]).astype(bf), over_lanes[...]).astype(bf)

        def backward(k, carry):
            tops = []
            for part in range(2):
                cotangent = sloped[...] * fields[k, pl.ds(part * points, points)]
                columns = dot(cotangent, grid_lanes_t[...]).astype(bf)
                tops.append(dot(grid_rows[...], columns))
            gather_adjoint(k, *tops, quads, acc)
            return carry

        lax.fori_loop(0, kernels, backward, 0, unroll=UNROLL)
        returned = dot(spectral_matrix(acc), outer_wide[...]).astype(bf)
        for first in (0, tile + AMBIT) + tuple(range(AMBIT, tile + AMBIT, AMBIT)):
            rows = pl.ds(first, AMBIT)
            piece = dot(outer_wide_t[rows], returned)
            edge = first in (0, tile + AMBIT)
            if now == 0:
                total[rows, pl.ds(0, extent)] = piece
                final = piece[:, :tile]
                if edge:
                    rim[rows, pl.ds(0, tile)] = final.astype(bf)
                else:
                    rim[rows, pl.ds(0, AMBIT)] = final[:, :AMBIT].astype(bf)
            else:
                both = total[rows, pl.ds(tile, extent - tile)] + piece[:, : extent - tile]
                total[rows, pl.ds(tile, extent - tile)] = both
                total[rows, pl.ds(extent, tile)] = piece[:, extent - tile :]
                if edge:
                    rim[rows, pl.ds(tile, extent - tile)] = both.astype(bf)
                    rim[rows, pl.ds(extent, tile)] = piece[:, extent - tile :].astype(bf)
                else:
                    rim[rows, pl.ds(width + AMBIT, AMBIT)] = piece[:, tile + AMBIT :].astype(bf)
        for slot, dr, dc, copy in back:
            if slot == now:
                only(dr, dc, copy.start)

    for now in range(2):
        for (slot, dr, dc, copy), entry in zip(back, rims(tile, width)):
            if slot != now:
                continue
            dst = entry[4]

            def add():
                copy.wait_recv()
                if dst[0] == "rows":
                    spot = (dst[1] * (tile - AMBIT), AMBIT, dst[2], dst[3])
                elif dst[0] == "cols":
                    spot = (0, tile, dst[1] * (width - AMBIT), AMBIT)
                else:
                    spot = (
                        dst[1] // 2 * (tile - AMBIT), AMBIT, dst[1] % 2 * (width - AMBIT), AMBIT)
                r, n, c, m = spot
                total[pl.ds(AMBIT + r, n), pl.ds(AMBIT + c, m)] += place(dst)[...].astype(jnp.float32)

            only(-dr, -dc, add)
    out[...] = total[pl.ds(AMBIT, tile), pl.ds(AMBIT, width)].astype(bf)
    for slot, dr, dc, copy in halo + back:
        only(dr, dc, copy.wait_send)


def body(grid, mask, target, live, pupils, weights):
    tile, width = mask.shape
    consts = tables(pupils.shape[2], tile)
    kernels = pupils.shape[1]
    bf, f32 = jnp.bfloat16, jnp.float32
    anywhere = pl.BlockSpec(memory_space=pl.ANY)
    smem = pl.BlockSpec(memory_space=pltpu.SMEM)
    extent = tile + 2 * AMBIT
    points, lanes = consts[10].shape[1], consts[3].shape[1]
    vmem = pl.BlockSpec(memory_space=pltpu.VMEM)
    gradient = pl.pallas_call(
        partial(kernel, grid),
        out_shape=jax.ShapeDtypeStruct(mask.shape, bf),
        in_specs=[smem, smem] + [anywhere] * (3 + len(consts)),
        out_specs=vmem,
        scratch_shapes=[pltpu.VMEM(t.shape, t.dtype) for t in consts]
        + [
            pltpu.VMEM((tile, width), f32),
            pltpu.VMEM((tile, width), bf),
            pltpu.VMEM(pupils.shape, f32),
            pltpu.VMEM((2, kernels, 2 * ROWS, 2 * LANES), f32),
            pltpu.VMEM((extent, width + 2 * AMBIT), bf),
            pltpu.VMEM((extent, width + 2 * AMBIT), f32),
            pltpu.VMEM((kernels, 2 * points, lanes), bf),
            pltpu.VMEM((points, lanes), f32),
            pltpu.VMEM((tile, tile), bf),
            pltpu.VMEM((points, lanes), bf),
            pltpu.VMEM((4, ROWS, LANES), f32),
            pltpu.VMEM((4, ROWS, LANES), f32),
            pltpu.VMEM(consts[2].shape[::-1], bf),
            pltpu.VMEM(consts[3].shape[::-1], bf),
            pltpu.VMEM(consts[7].shape[::-1], bf),
            pltpu.VMEM((points, lanes), bf),
            pltpu.VMEM((points, lanes), bf),
            pltpu.VMEM((extent, width + 2 * AMBIT), bf),
            pltpu.VMEM((2, AMBIT, width), bf),
            pltpu.VMEM((2, tile, AMBIT), bf),
            pltpu.VMEM((4, AMBIT, AMBIT), bf),
            pltpu.SemaphoreType.DMA((5 + len(consts),)),
        ]
        + [pltpu.SemaphoreType.DMA((10,))] * 4,
        compiler_params=pltpu.CompilerParams(
            collective_id=0, has_side_effects=True, vmem_limit_bytes=VMEM_LIMIT
        ),
    )(live, weights, mask, target, pupils, *consts)
    return mask - step_rate * gradient.astype(f32)


def solution(mesh):
    return jax.shard_map(
        partial(body, (mesh.shape["row"], mesh.shape["col"])),
        mesh=mesh,
        in_specs=(P("row", "col"), P("row", "col"), P("row", "col"), P(), P()),
        out_specs=P("row", "col"),
        check_vma=False,
    )
```

```python
from functools import partial
import math

import jax
import jax.numpy as jnp
import numpy as np
from jax import lax
from jax.experimental import pallas as pl
from jax.experimental.pallas import tpu as pltpu
from jax.sharding import PartitionSpec as P

AMBIT = 128
ROWS = 80
LANES = 128

steepness = 4.0
threshold_level = 1.0
step_rate = 8.0

UNROLL = 2
VMEM_LIMIT = 60 * 1024 * 1024


def folded(count, pixels, offset, period, pad):
    half = count // 2
    frequency = np.arange(half + 1)
    place = np.arange(pixels) + offset
    phases = np.mod(frequency[:, None] * place[None, :], period).astype(np.float32)
    angles = phases * np.float32(2.0 * math.pi / period)
    factor = np.float32(1.0 / math.sqrt(period))
    table = np.zeros((2, pad, pixels), np.float32)
    table[0, : half + 1] = np.cos(angles) * factor
    table[1, : half + 1] = np.sin(angles) * factor
    return table.reshape(2 * pad, pixels)


def grid_table(count, points, period, pad):
    half = count // 2
    angles = np.arange(half + 1)[:, None] * np.arange(points)[None, :] * (2.0 * math.pi / points)
    table = np.zeros((2, pad, points))
    table[0, : half + 1] = np.cos(angles) / math.sqrt(period)
    table[1, : half + 1] = np.sin(angles) / math.sqrt(period)
    return table.reshape(2 * pad, points)


def between(count, points, pixels, offset, period):
    gap = np.arange(pixels)[:, None] + offset - np.arange(points)[None, :] * (period / points)
    gap = gap * (2.0 * math.pi / period)
    return (1.0 + 2.0 * sum(np.cos(m * gap) for m in range(1, count + 1))) / points


def halves(table):
    high = table.astype(jnp.bfloat16).astype(np.float64)
    return high, table - high


def tables(count, tile):
    extent = tile + 2 * AMBIT
    rows = -(-(2 * count + 1) // 16) * 16
    lanes = -(-(2 * count + 1) // 128) * 128
    grid_rows = grid_table(count, rows, extent, ROWS)
    grid_lanes = grid_table(count, lanes, extent, LANES)
    over_rows = between(count, rows, tile, AMBIT, extent)
    over_lanes = between(count, lanes, tile, AMBIT, extent)
    outer_wide = folded(count, extent, 0, extent, LANES)
    half = count // 2
    left = np.zeros((2 * ROWS, count), np.float32)
    right = np.zeros((2 * LANES, count), np.float32)
    for table, pad in ((left, ROWS), (right, LANES)):
        for f in range(half + 1):
            if f < half:
                table[f, half + f] = 1.0
            if f > 0:
                table[pad + f, half - f] = 1.0
    rows_high, rows_low = halves(over_rows)
    lanes_high, lanes_low = halves(over_lanes.T)
    return [
        jnp.asarray(t, jnp.bfloat16)
        for t in (
            left, right.T, outer_wide, grid_lanes, grid_rows.T, rows_high, rows_low, lanes_high,
            lanes_low, grid_rows,
        )
    ]


def dot(a, b):
    return jnp.dot(a, b, preferred_element_type=jnp.float32)


def split(value):
    upper = value.astype(jnp.bfloat16)
    return upper, (value - upper.astype(jnp.float32)).astype(jnp.bfloat16)


def times(ar, ai, br, bi):
    return ar * br - ai * bi, ar * bi + ai * br


def quarter(ref, part, k):
    return (
        ref[part, k, :ROWS, :LANES],
        ref[part, k, :ROWS, LANES:],
        ref[part, k, ROWS:, :LANES],
        ref[part, k, ROWS:, LANES:],
    )


def fold_pupils(pupils, weights, left, right, quads):
    bf = jnp.bfloat16

    def one(k, carry):
        root = jnp.sqrt(jnp.full((1, pupils.shape[3]), weights[k], jnp.float32))
        for part in range(2):
            value = pupils[part, k] * root
            moved = [dot(left[...], dot(v, right[...]).astype(bf)) for v in split(value)]
            quads[part, k] = moved[0] + moved[1]
        return carry

    lax.fori_loop(0, pupils.shape[1], one, 0)


def take_spectrum(window, outer_wide, outer_wide_t, spec):
    bf = jnp.bfloat16
    folds = jnp.concatenate([outer_wide[:ROWS], outer_wide[LANES : LANES + ROWS]], axis=0)
    partial_rows = dot(folds, window).astype(bf)
    blocks = dot(partial_rows, outer_wide_t[...])
    cc, cs = blocks[:ROWS, :LANES], blocks[:ROWS, LANES:]
    sc, ss = blocks[ROWS:, :LANES], blocks[ROWS:, LANES:]
    spec[0] = (cc - ss).astype(bf).astype(jnp.float32)
    spec[1] = -((cs + sc).astype(bf).astype(jnp.float32))
    spec[2] = (cc + ss).astype(bf).astype(jnp.float32)
    spec[3] = (cs - sc).astype(bf).astype(jnp.float32)


def amplitude_of(k, quads, spec):
    ar, br, cr, dr = quarter(quads, 0, k)
    ai, bi, ci, di = quarter(quads, 1, k)
    z1r, z1i, z2r, z2i = spec[0], spec[1], spec[2], spec[3]
    ppr, ppi = times(ar, ai, z1r, z1i)
    pnr, pni = times(br, bi, z2r, z2i)
    npr, npi = times(cr, ci, z2r, -z2i)
    nnr, nni = times(dr, di, z1r, -z1i)
    pr, pi, mr, mi = ppr + nnr, ppi + nni, ppr - nnr, ppi - nni
    qr, qi, nr, ni = pnr + npr, pni + npi, pnr - npr, pni - npi
    return jnp.concatenate(
        [
            jnp.concatenate([pr + qr, ni - mi], axis=1),
            jnp.concatenate([-(mi + ni), qr - pr], axis=1),
            jnp.concatenate([pi + qi, mr - nr], axis=1),
            jnp.concatenate([mr + nr, qi - pi], axis=1),
        ],
        axis=0,
    ).astype(jnp.bfloat16)


def gather_adjoint(k, re, im, quads, acc):
    ar, br, cr, dr = quarter(quads, 0, k)
    ai, bi, ci, di = quarter(quads, 1, k)
    ccr, csr, scr, ssr = re[:ROWS, :LANES], re[:ROWS, LANES:], re[ROWS:, :LANES], re[ROWS:, LANES:]
    cci, csi, sci, ssi = im[:ROWS, :LANES], im[:ROWS, LANES:], im[ROWS:, :LANES], im[ROWS:, LANES:]
    er, ei, fr, fi = ccr - ssr, cci - ssi, ccr + ssr, cci + ssi
    gr, gi, hr, hi = csr + scr, csi + sci, csr - scr, csi - sci
    ur, ui = times(ar, -ai, er + gi, ei - gr)
    vr, vi = times(dr, di, er - gi, -(ei + gr))
    acc[0] += ur + vr
    acc[1] += ui + vi
    ur, ui = times(br, -bi, fr - hi, fi + hr)
    vr, vi = times(cr, ci, fr + hi, hr - fi)
    acc[2] += ur + vr
    acc[3] += ui + vi


def spectral_matrix(acc):
    u1r, u1i, u2r, u2i = acc[0], acc[1], acc[2], acc[3]
    rest = jnp.zeros((LANES - ROWS, 2 * LANES), jnp.float32)
    return jnp.concatenate(
        [
            jnp.concatenate([u1r + u2r, u2i - u1i], axis=1),
            rest,
            jnp.concatenate([-(u1i + u2i), u2r - u1r], axis=1),
            rest,
        ],
        axis=0,
    ).astype(jnp.bfloat16)


def pieces(tile, width):
    low, high = tile + AMBIT, width + AMBIT
    split = tile + 2 * AMBIT
    rows = {-1: ((AMBIT, AMBIT), low), 0: ((AMBIT, tile), AMBIT), 1: ((tile, AMBIT), 0)}
    outs = []
    for slot in range(2):
        for dr in (-1, 1, 0):
            (first, count), place = rows[dr]
            if dr:
                c0, c1 = ((AMBIT, split), (split, high))[slot]
                outs.append((slot, dr, 0, (first, count, c0, c1 - c0), (place, count, c0, c1 - c0)))
            if slot == 0:
                outs.append((0, dr, 1, (first, count, width, AMBIT), (place, count, 0, AMBIT)))
            else:
                outs.append((1, dr, -1, (first, count, AMBIT, AMBIT), (place, count, high, AMBIT)))
    return outs


def rims(tile, width):
    low, high = tile + AMBIT, width + AMBIT
    cut = tile - AMBIT
    outs = []
    for slot in range(2):
        for dr in (-1, 1, 0):
            first, count = ((AMBIT, tile), (low, AMBIT), (0, AMBIT))[dr]
            side = 1 if dr < 0 else 0
            if dr:
                c0, c1 = ((AMBIT, tile), (tile, high))[slot]
                outs.append((slot, dr, 0, (first, count, c0, c1 - c0), ("rows", side, c0 - AMBIT, c1 - c0)))
            dc, c0, other = ((-1, 0, 1), (1, high, 0))[slot]
            if dr:
                outs.append((slot, dr, dc, (first, count, c0, AMBIT), ("corner", 2 * side + other)))
            else:
                outs.append((slot, 0, dc, (first, count, c0, AMBIT), ("cols", other)))
    return outs


def window(ref, place):
    row, rows, col, cols = place
    return ref.at[pl.ds(row, rows), pl.ds(col, cols)]


def kernel(
    grid, live_ref, weight_ref, mask_hbm, goal_hbm, pupil_hbm, *refs,
):
    tables_hbm, refs = refs[:10], refs[10:]
    out = refs[0]
    held, refs = refs[1:11], refs[11:]
    (
        mask, goal, pupils, quads, ext, total, fields, intensity, slope, sloped, spec, acc,
        outer_wide_t, grid_lanes_t, over_lanes, over_rows_t, high, low, rim, got_rows, got_cols, got_corner, in_sem, halo_send, halo_recv, rim_send, rim_recv,
    ) = refs
    (
        left, right, outer_wide, grid_lanes, grid_rows_t, rows_high, rows_low, lanes_high,
        lanes_low, grid_rows,
    ) = held
    bf = jnp.bfloat16
    tile, width = mask.shape
    extent = tile + 2 * AMBIT
    kernels = pupils.shape[1]
    row, col = lax.axis_index("row"), lax.axis_index("col")
    last_row, last_col = grid[0] - 1, grid[1] - 1

    def there(dr, dc):
        ok = jnp.bool_(True)
        if dr:
            ok = row > 0 if dr < 0 else row < last_row
        if dc:
            side = col > 0 if dc < 0 else col < last_col
            ok = jnp.logical_and(ok, side) if dr else side
        return ok

    def only(dr, dc, act):
        pl.when(there(dr, dc))(act)

    cuts = ((0, AMBIT), (tile - AMBIT, AMBIT), (AMBIT, tile - 2 * AMBIT))
    loads = [
        pltpu.make_async_copy(mask_hbm.at[pl.ds(a, n)], mask.at[pl.ds(a, n)], in_sem.at[i])
        for i, (a, n) in enumerate(cuts)
    ]
    loads.append(pltpu.make_async_copy(pupil_hbm, pupils, in_sem.at[3]))
    first_table = len(loads)
    for source, target in zip(tables_hbm, held):
        loads.append(pltpu.make_async_copy(source, target, in_sem.at[len(loads)]))
    goal_load = len(loads)
    loads.append(pltpu.make_async_copy(goal_hbm, goal, in_sem.at[goal_load]))
    for load in loads:
        load.start()

    barrier = pltpu.get_barrier_semaphore()
    around = [(dr, dc) for dr in (-1, 0, 1) for dc in (-1, 0, 1) if dr or dc]
    for dr, dc in around:
        only(dr, dc, lambda: pl.semaphore_signal(
            barrier, inc=1, device_id=(row + dr, col + dc), device_id_type=pl.DeviceIdType.MESH))
    for i, (a, n) in enumerate(cuts):
        loads[i].wait()
        ext[pl.ds(AMBIT + a, n), pl.ds(AMBIT, width)] = mask[pl.ds(a, n)].astype(bf)
    tall = 3 - (row == 0).astype(jnp.int32) - (row == last_row).astype(jnp.int32)
    broad = 3 - (col == 0).astype(jnp.int32) - (col == last_col).astype(jnp.int32)
    pl.semaphore_wait(barrier, tall * broad - 1)

    def copies(table, source, target, send, recv):
        outs = []
        for i, (slot, dr, dc, src, dst) in enumerate(table):
            outs.append((slot, dr, dc, pltpu.make_async_remote_copy(
                src_ref=window(source, src), dst_ref=target(dst), send_sem=send.at[i],
                recv_sem=recv.at[i], device_id=(row + dr, col + dc),
                device_id_type=pl.DeviceIdType.MESH)))
        return outs

    def place(dst):
        if dst[0] == "rows":
            return got_rows.at[dst[1], :, pl.ds(dst[2], dst[3])]
        return got_cols.at[dst[1]] if dst[0] == "cols" else got_corner.at[dst[1]]

    halo = copies(pieces(tile, width), ext, lambda dst: window(ext, dst), halo_send, halo_recv)
    back = copies(rims(tile, width), rim, place, rim_send, rim_recv)
    for slot, dr, dc, copy in halo:
        only(dr, dc, copy.start)
    for slot, dr, dc, src, dst in pieces(tile, width):

        def clear():
            ext[pl.ds(dst[0], dst[1]), pl.ds(dst[2], dst[3])] = jnp.zeros((dst[1], dst[3]), bf)

        pl.when(jnp.logical_not(there(-dr, -dc)))(clear)

    loads[3].wait()
    for load in loads[first_table : first_table + 2]:
        load.wait()
    fold_pupils(pupils, weight_ref, left, right, quads)
    for load in loads[first_table + 2 :]:
        load.wait()
    points = grid_rows.shape[1]
    outer_wide_t[...] = outer_wide[...].T
    grid_lanes_t[...] = grid_lanes[...].T
    over_lanes[...] = lanes_high[...].T
    over_rows_t[...] = rows_high[...].T

    for now in range(2):
        for slot, dr, dc, copy in halo:
            if slot == now:
                only(-dr, -dc, copy.wait_recv)
        base = now * tile
        take_spectrum(ext[:, pl.ds(base, extent)], outer_wide, outer_wide_t, spec)
        intensity[...] = jnp.zeros_like(intensity)
        acc[...] = jnp.zeros_like(acc)

        def forward(k, carry):
            section = dot(amplitude_of(k, quads, spec), grid_lanes[...]).astype(bf)
            both = jnp.concatenate([section[: 2 * ROWS], section[2 * ROWS :]], axis=1)
            field = dot(grid_rows_t[...], both)
            lanes = grid_lanes.shape[1]
            field_re, field_im = field[:, :lanes], field[:, lanes:]
            intensity[...] += field_re * field_re + field_im * field_im
            fields[k, :points] = field_re.astype(bf)
            fields[k, points:] = field_im.astype(bf)
            return carry

        lax.fori_loop(0, kernels, forward, 0, unroll=UNROLL)
        high[...], low[...] = split(intensity[...])
        live = live_ref[0, now].astype(jnp.float32)
        for first in range(0, tile, 128):
            rows = pl.ds(first, 128)
            level = dot(rows_high[rows], high[...]) + dot(rows_high[rows], low[...])
            level = level + dot(rows_low[rows], high[...])
            upper, lower = split(level)
            level = dot(upper, lanes_high[...]) + dot(lower, lanes_high[...])
            level = level + dot(upper, lanes_low[...])
            resist = 1.0 / (1.0 + jnp.exp(-steepness * (level - threshold_level)))
            wanted = goal[rows, pl.ds(base, tile)].astype(jnp.float32)
            slope[rows] = (
                (2.0 * steepness * live) * (resist - wanted) * resist * (1.0 - resist)
            ).astype(bf)
        sloped[...] = dot(dot(over_rows_t[...], slope[...]).astype(bf), over_lanes[...]).astype(bf)

        def backward(k, carry):
            weight = sloped[...]
            cotangent = jnp.concatenate(
                [weight * fields[k, :points], weight * fields[k, points:]], axis=0)
            columns = dot(cotangent, grid_lanes_t[...]).astype(bf)
            columns = jnp.concatenate([columns[:points], columns[points:]], axis=1)
            top = dot(grid_rows[...], columns)
            tops = [top[:, : 2 * LANES], top[:, 2 * LANES :]]
            gather_adjoint(k, *tops, quads, acc)
            return carry

        lax.fori_loop(0, kernels, backward, 0, unroll=UNROLL)
        returned = dot(spectral_matrix(acc), outer_wide[...]).astype(bf)
        for first in (0, tile + AMBIT) + tuple(range(AMBIT, tile + AMBIT, AMBIT)):
            rows = pl.ds(first, AMBIT)
            piece = dot(outer_wide_t[rows], returned)
            edge = first in (0, tile + AMBIT)
            if now == 0:
                total[rows, pl.ds(0, extent)] = piece
                final = piece[:, :tile]
                if edge:
                    rim[rows, pl.ds(0, tile)] = final.astype(bf)
                else:
                    rim[rows, pl.ds(0, AMBIT)] = final[:, :AMBIT].astype(bf)
            else:
                both = total[rows, pl.ds(tile, extent - tile)] + piece[:, : extent - tile]
                total[rows, pl.ds(tile, extent - tile)] = both
                total[rows, pl.ds(extent, tile)] = piece[:, extent - tile :]
                if edge:
                    rim[rows, pl.ds(tile, extent - tile)] = both.astype(bf)
                    rim[rows, pl.ds(extent, tile)] = piece[:, extent - tile :].astype(bf)
                else:
                    rim[rows, pl.ds(width + AMBIT, AMBIT)] = piece[:, tile + AMBIT :].astype(bf)
        for slot, dr, dc, copy in back:
            if slot == now:
                only(dr, dc, copy.start)

    for now in range(2):
        for (slot, dr, dc, copy), entry in zip(back, rims(tile, width)):
            if slot != now:
                continue
            dst = entry[4]

            def add():
                copy.wait_recv()
                if dst[0] == "rows":
                    spot = (dst[1] * (tile - AMBIT), AMBIT, dst[2], dst[3])
                elif dst[0] == "cols":
                    spot = (0, tile, dst[1] * (width - AMBIT), AMBIT)
                else:
                    spot = (
                        dst[1] // 2 * (tile - AMBIT), AMBIT, dst[1] % 2 * (width - AMBIT), AMBIT)
                r, n, c, m = spot
                total[pl.ds(AMBIT + r, n), pl.ds(AMBIT + c, m)] += place(dst)[...].astype(jnp.float32)

            only(-dr, -dc, add)
    out[...] = total[pl.ds(AMBIT, tile), pl.ds(AMBIT, width)].astype(bf)
    for slot, dr, dc, copy in halo + back:
        only(dr, dc, copy.wait_send)


def body(grid, mask, target, live, pupils, weights):
    tile, width = mask.shape
    consts = tables(pupils.shape[2], tile)
    kernels = pupils.shape[1]
    bf, f32 = jnp.bfloat16, jnp.float32
    anywhere = pl.BlockSpec(memory_space=pl.ANY)
    smem = pl.BlockSpec(memory_space=pltpu.SMEM)
    extent = tile + 2 * AMBIT
    points, lanes = consts[9].shape[1], consts[3].shape[1]
    vmem = pl.BlockSpec(memory_space=pltpu.VMEM)
    gradient = pl.pallas_call(
        partial(kernel, grid),
        out_shape=jax.ShapeDtypeStruct(mask.shape, bf),
        in_specs=[smem, smem] + [anywhere] * (3 + len(consts)),
        out_specs=vmem,
        scratch_shapes=[pltpu.VMEM(t.shape, t.dtype) for t in consts]
        + [
            pltpu.VMEM((tile, width), f32),
            pltpu.VMEM((tile, width), bf),
            pltpu.VMEM(pupils.shape, f32),
            pltpu.VMEM((2, kernels, 2 * ROWS, 2 * LANES), f32),
            pltpu.VMEM((extent, width + 2 * AMBIT), bf),
            pltpu.VMEM((extent, width + 2 * AMBIT), f32),
            pltpu.VMEM((kernels, 2 * points, lanes), bf),
            pltpu.VMEM((points, lanes), f32),
            pltpu.VMEM((tile, tile), bf),
            pltpu.VMEM((points, lanes), bf),
            pltpu.VMEM((4, ROWS, LANES), f32),
            pltpu.VMEM((4, ROWS, LANES), f32),
            pltpu.VMEM(consts[2].shape[::-1], bf),
            pltpu.VMEM(consts[3].shape[::-1], bf),
            pltpu.VMEM(consts[7].shape[::-1], bf),
            pltpu.VMEM(consts[5].shape[::-1], bf),
            pltpu.VMEM((points, lanes), bf),
            pltpu.VMEM((points, lanes), bf),
            pltpu.VMEM((extent, width + 2 * AMBIT), bf),
            pltpu.VMEM((2, AMBIT, width), bf),
            pltpu.VMEM((2, tile, AMBIT), bf),
            pltpu.VMEM((4, AMBIT, AMBIT), bf),
            pltpu.SemaphoreType.DMA((5 + len(consts),)),
        ]
        + [pltpu.SemaphoreType.DMA((10,))] * 4,
        compiler_params=pltpu.CompilerParams(
            collective_id=0, has_side_effects=True, vmem_limit_bytes=VMEM_LIMIT
        ),
    )(live, weights, mask, target, pupils, *consts)
    return mask - step_rate * gradient.astype(f32)


def solution(mesh):
    return jax.shard_map(
        partial(body, (mesh.shape["row"], mesh.shape["col"])),
        mesh=mesh,
        in_specs=(P("row", "col"), P("row", "col"), P("row", "col"), P(), P()),
        out_specs=P("row", "col"),
        check_vma=False,
    )
```

```python
from functools import partial
import math

import jax
import jax.numpy as jnp
import numpy as np
from jax import lax
from jax.experimental import pallas as pl
from jax.experimental.pallas import tpu as pltpu
from jax.sharding import PartitionSpec as P

AMBIT = 128
ROWS = 80
LANES = 128

steepness = 4.0
threshold_level = 1.0
step_rate = 8.0

UNROLL = 6
VMEM_LIMIT = 60 * 1024 * 1024


def folded(count, pixels, offset, period, pad):
    half = count // 2
    frequency = np.arange(half + 1)
    place = np.arange(pixels) + offset
    phases = np.mod(frequency[:, None] * place[None, :], period).astype(np.float32)
    angles = phases * np.float32(2.0 * math.pi / period)
    factor = np.float32(1.0 / math.sqrt(period))
    table = np.zeros((2, pad, pixels), np.float32)
    table[0, : half + 1] = np.cos(angles) * factor
    table[1, : half + 1] = np.sin(angles) * factor
    return table.reshape(2 * pad, pixels)


def grid_table(count, points, period, pad):
    half = count // 2
    angles = np.arange(half + 1)[:, None] * np.arange(points)[None, :] * (2.0 * math.pi / points)
    table = np.zeros((2, pad, points))
    table[0, : half + 1] = np.cos(angles) / math.sqrt(period)
    table[1, : half + 1] = np.sin(angles) / math.sqrt(period)
    return table.reshape(2 * pad, points)


def between(count, points, pixels, offset, period):
    gap = np.arange(pixels)[:, None] + offset - np.arange(points)[None, :] * (period / points)
    gap = gap * (2.0 * math.pi / period)
    return (1.0 + 2.0 * sum(np.cos(m * gap) for m in range(1, count + 1))) / points


def halves(table):
    high = table.astype(jnp.bfloat16).astype(np.float64)
    return high, table - high


def tables(count, tile):
    extent = tile + 2 * AMBIT
    rows = -(-(2 * count + 1) // 16) * 16
    lanes = -(-(2 * count + 1) // 128) * 128
    grid_rows = grid_table(count, rows, extent, ROWS)
    grid_lanes = grid_table(count, lanes, extent, LANES)
    over_rows = between(count, rows, tile, AMBIT, extent)
    over_lanes = between(count, lanes, tile, AMBIT, extent)
    outer_wide = folded(count, extent, 0, extent, LANES)
    rows_high, rows_low = halves(over_rows)
    lanes_high, lanes_low = halves(over_lanes.T)
    return [
        jnp.asarray(t, jnp.bfloat16)
        for t in (
            outer_wide, grid_lanes, grid_rows.T, rows_high, rows_low, lanes_high, lanes_low,
            grid_rows,
        )
    ]


def dot(a, b):
    return jnp.dot(a, b, preferred_element_type=jnp.float32)


def split(value):
    upper = value.astype(jnp.bfloat16)
    return upper, (value - upper.astype(jnp.float32)).astype(jnp.bfloat16)


def times(ar, ai, br, bi):
    return ar * br - ai * bi, ar * bi + ai * br


def quarter(ref, part, k):
    return (
        ref[part, k, :ROWS, :LANES],
        ref[part, k, :ROWS, LANES:],
        ref[part, k, ROWS:, :LANES],
        ref[part, k, ROWS:, LANES:],
    )


def one_hot(shape, half, pad, along):
    place = lax.broadcasted_iota(jnp.int32, shape, along)
    source = lax.broadcasted_iota(jnp.int32, shape, 1 - along)
    above = place >= pad
    wanted = jnp.where(above, half + pad - place, half + place)
    hit = jnp.logical_and(source == wanted, place != pad)
    return jnp.where(hit, 1.0, 0.0).astype(jnp.bfloat16)


def fold_pupils(pupils, weights, quads):
    bf = jnp.bfloat16
    count = pupils.shape[3]
    left = one_hot((2 * ROWS, count), count // 2, ROWS, 0)
    right = one_hot((count, 2 * LANES), count // 2, LANES, 1)

    def one(k, carry):
        root = jnp.sqrt(jnp.full((1, pupils.shape[3]), weights[k], jnp.float32))
        for part in range(2):
            value = pupils[part, k] * root
            moved = [dot(left, dot(v, right).astype(bf)) for v in split(value)]
            quads[part, k] = moved[0] + moved[1]
        return carry

    lax.fori_loop(0, pupils.shape[1], one, 0)


def take_spectrum(window, outer_wide, outer_wide_t, spec):
    bf = jnp.bfloat16
    folds = jnp.concatenate([outer_wide[:ROWS], outer_wide[LANES : LANES + ROWS]], axis=0)
    partial_rows = dot(folds, window).astype(bf)
    blocks = dot(partial_rows, outer_wide_t[...])
    cc, cs = blocks[:ROWS, :LANES], blocks[:ROWS, LANES:]
    sc, ss = blocks[ROWS:, :LANES], blocks[ROWS:, LANES:]
    spec[0] = (cc - ss).astype(bf).astype(jnp.float32)
    spec[1] = -((cs + sc).astype(bf).astype(jnp.float32))
    spec[2] = (cc + ss).astype(bf).astype(jnp.float32)
    spec[3] = (cs - sc).astype(bf).astype(jnp.float32)


def amplitude_of(k, quads, spec):
    ar, br, cr, dr = quarter(quads, 0, k)
    ai, bi, ci, di = quarter(quads, 1, k)
    z1r, z1i, z2r, z2i = spec[0], spec[1], spec[2], spec[3]
    ppr, ppi = times(ar, ai, z1r, z1i)
    pnr, pni = times(br, bi, z2r, z2i)
    npr, npi = times(cr, ci, z2r, -z2i)
    nnr, nni = times(dr, di, z1r, -z1i)
    pr, pi, mr, mi = ppr + nnr, ppi + nni, ppr - nnr, ppi - nni
    qr, qi, nr, ni = pnr + npr, pni + npi, pnr - npr, pni - npi
    return jnp.concatenate(
        [
            jnp.concatenate([pr + qr, ni - mi], axis=1),
            jnp.concatenate([-(mi + ni), qr - pr], axis=1),
            jnp.concatenate([pi + qi, mr - nr], axis=1),
            jnp.concatenate([mr + nr, qi - pi], axis=1),
        ],
        axis=0,
    ).astype(jnp.bfloat16)


def gather_adjoint(k, re, im, quads, acc):
    ar, br, cr, dr = quarter(quads, 0, k)
    ai, bi, ci, di = quarter(quads, 1, k)
    ccr, csr, scr, ssr = re[:ROWS, :LANES], re[:ROWS, LANES:], re[ROWS:, :LANES], re[ROWS:, LANES:]
    cci, csi, sci, ssi = im[:ROWS, :LANES], im[:ROWS, LANES:], im[ROWS:, :LANES], im[ROWS:, LANES:]
    er, ei, fr, fi = ccr - ssr, cci - ssi, ccr + ssr, cci + ssi
    gr, gi, hr, hi = csr + scr, csi + sci, csr - scr, csi - sci
    ur, ui = times(ar, -ai, er + gi, ei - gr)
    vr, vi = times(dr, di, er - gi, -(ei + gr))
    acc[0] += ur + vr
    acc[1] += ui + vi
    ur, ui = times(br, -bi, fr - hi, fi + hr)
    vr, vi = times(cr, ci, fr + hi, hr - fi)
    acc[2] += ur + vr
    acc[3] += ui + vi


def spectral_matrix(acc):
    u1r, u1i, u2r, u2i = acc[0], acc[1], acc[2], acc[3]
    rest = jnp.zeros((LANES - ROWS, 2 * LANES), jnp.float32)
    return jnp.concatenate(
        [
            jnp.concatenate([u1r + u2r, u2i - u1i], axis=1),
            rest,
            jnp.concatenate([-(u1i + u2i), u2r - u1r], axis=1),
            rest,
        ],
        axis=0,
    ).astype(jnp.bfloat16)


def pieces(tile, width):
    low, high = tile + AMBIT, width + AMBIT
    split = tile + 2 * AMBIT
    rows = {-1: ((AMBIT, AMBIT), low), 0: ((AMBIT, tile), AMBIT), 1: ((tile, AMBIT), 0)}
    outs = []
    for slot in range(2):
        for dr in (-1, 1, 0):
            (first, count), place = rows[dr]
            if dr:
                c0, c1 = ((AMBIT, split), (split, high))[slot]
                outs.append((slot, dr, 0, (first, count, c0, c1 - c0), (place, count, c0, c1 - c0)))
            if slot == 0:
                outs.append((0, dr, 1, (first, count, width, AMBIT), (place, count, 0, AMBIT)))
            else:
                outs.append((1, dr, -1, (first, count, AMBIT, AMBIT), (place, count, high, AMBIT)))
    return outs


def rims(tile, width):
    low, high = tile + AMBIT, width + AMBIT
    cut = tile - AMBIT
    outs = []
    for slot in range(2):
        for dr in (-1, 1, 0):
            first, count = ((AMBIT, tile), (low, AMBIT), (0, AMBIT))[dr]
            side = 1 if dr < 0 else 0
            if dr:
                c0, c1 = ((AMBIT, tile), (tile, high))[slot]
                outs.append((slot, dr, 0, (first, count, c0, c1 - c0), ("rows", side, c0 - AMBIT, c1 - c0)))
            dc, c0, other = ((-1, 0, 1), (1, high, 0))[slot]
            if dr:
                outs.append((slot, dr, dc, (first, count, c0, AMBIT), ("corner", 2 * side + other)))
            else:
                outs.append((slot, 0, dc, (first, count, c0, AMBIT), ("cols", other)))
    return outs


def window(ref, place):
    row, rows, col, cols = place
    return ref.at[pl.ds(row, rows), pl.ds(col, cols)]


def kernel(
    grid, live_ref, weight_ref, mask_hbm, goal_hbm, pupil_hbm, *refs,
):
    tables_hbm, refs = refs[:8], refs[8:]
    out = refs[0]
    held, refs = refs[1:9], refs[9:]
    (
        mask, goal, pupils, quads, ext, total, fields, intensity, slope, sloped, spec, acc,
        outer_wide_t, grid_lanes_t, over_lanes, over_rows_t, high, low, rim, got_rows, got_cols, got_corner, in_sem, halo_send, halo_recv, rim_send, rim_recv,
    ) = refs
    (
        outer_wide, grid_lanes, grid_rows_t, rows_high, rows_low, lanes_high, lanes_low, grid_rows,
    ) = held
    bf = jnp.bfloat16
    tile, width = mask.shape
    extent = tile + 2 * AMBIT
    kernels = pupils.shape[1]
    row, col = lax.axis_index("row"), lax.axis_index("col")
    last_row, last_col = grid[0] - 1, grid[1] - 1

    def there(dr, dc):
        ok = jnp.bool_(True)
        if dr:
            ok = row > 0 if dr < 0 else row < last_row
        if dc:
            side = col > 0 if dc < 0 else col < last_col
            ok = jnp.logical_and(ok, side) if dr else side
        return ok

    def only(dr, dc, act):
        pl.when(there(dr, dc))(act)

    cuts = ((0, AMBIT), (tile - AMBIT, AMBIT), (AMBIT, tile - 2 * AMBIT))
    loads = [
        pltpu.make_async_copy(mask_hbm.at[pl.ds(a, n)], mask.at[pl.ds(a, n)], in_sem.at[i])
        for i, (a, n) in enumerate(cuts)
    ]
    loads.append(pltpu.make_async_copy(pupil_hbm, pupils, in_sem.at[3]))
    first_table = len(loads)
    for source, target in zip(tables_hbm, held):
        loads.append(pltpu.make_async_copy(source, target, in_sem.at[len(loads)]))
    goal_load = len(loads)
    loads.append(pltpu.make_async_copy(goal_hbm, goal, in_sem.at[goal_load]))
    for load in loads:
        load.start()

    barrier = pltpu.get_barrier_semaphore()
    around = [(dr, dc) for dr in (-1, 0, 1) for dc in (-1, 0, 1) if dr or dc]
    for dr, dc in around:
        only(dr, dc, lambda: pl.semaphore_signal(
            barrier, inc=1, device_id=(row + dr, col + dc), device_id_type=pl.DeviceIdType.MESH))
    for i, (a, n) in enumerate(cuts):
        loads[i].wait()
        ext[pl.ds(AMBIT + a, n), pl.ds(AMBIT, width)] = mask[pl.ds(a, n)].astype(bf)
    tall = 3 - (row == 0).astype(jnp.int32) - (row == last_row).astype(jnp.int32)
    broad = 3 - (col == 0).astype(jnp.int32) - (col == last_col).astype(jnp.int32)
    pl.semaphore_wait(barrier, tall * broad - 1)

    def copies(table, source, target, send, recv):
        outs = []
        for i, (slot, dr, dc, src, dst) in enumerate(table):
            outs.append((slot, dr, dc, pltpu.make_async_remote_copy(
                src_ref=window(source, src), dst_ref=target(dst), send_sem=send.at[i],
                recv_sem=recv.at[i], device_id=(row + dr, col + dc),
                device_id_type=pl.DeviceIdType.MESH)))
        return outs

    def place(dst):
        if dst[0] == "rows":
            return got_rows.at[dst[1], :, pl.ds(dst[2], dst[3])]
        return got_cols.at[dst[1]] if dst[0] == "cols" else got_corner.at[dst[1]]

    halo = copies(pieces(tile, width), ext, lambda dst: window(ext, dst), halo_send, halo_recv)
    back = copies(rims(tile, width), rim, place, rim_send, rim_recv)
    for slot, dr, dc, copy in halo:
        only(dr, dc, copy.start)
    for slot, dr, dc, src, dst in pieces(tile, width):

        def clear():
            ext[pl.ds(dst[0], dst[1]), pl.ds(dst[2], dst[3])] = jnp.zeros((dst[1], dst[3]), bf)

        pl.when(jnp.logical_not(there(-dr, -dc)))(clear)

    loads[3].wait()
    fold_pupils(pupils, weight_ref, quads)
    for load in loads[first_table:]:
        load.wait()
    points = grid_rows.shape[1]
    outer_wide_t[...] = outer_wide[...].T
    grid_lanes_t[...] = grid_lanes[...].T
    over_lanes[...] = lanes_high[...].T
    over_rows_t[...] = rows_high[...].T

    for now in range(2):
        for slot, dr, dc, copy in halo:
            if slot == now:
                only(-dr, -dc, copy.wait_recv)
        base = now * tile
        take_spectrum(ext[:, pl.ds(base, extent)], outer_wide, outer_wide_t, spec)
        intensity[...] = jnp.zeros_like(intensity)
        acc[...] = jnp.zeros_like(acc)

        def forward(k, carry):
            section = dot(amplitude_of(k, quads, spec), grid_lanes[...]).astype(bf)
            both = jnp.concatenate([section[: 2 * ROWS], section[2 * ROWS :]], axis=1)
            field = dot(grid_rows_t[...], both)
            lanes = grid_lanes.shape[1]
            field_re, field_im = field[:, :lanes], field[:, lanes:]
            intensity[...] += field_re * field_re + field_im * field_im
            fields[k, :points] = field_re.astype(bf)
            fields[k, points:] = field_im.astype(bf)
            return carry

        lax.fori_loop(0, kernels, forward, 0, unroll=UNROLL)
        high[...], low[...] = split(intensity[...])
        live = live_ref[0, now].astype(jnp.float32)
        def compare(part, carry):
            rows = pl.ds(pl.multiple_of(part * 128, 128), 128)
            level = dot(rows_high[rows], high[...]) + dot(rows_high[rows], low[...])
            level = level + dot(rows_low[rows], high[...])
            upper, lower = split(level)
            level = dot(upper, lanes_high[...]) + dot(lower, lanes_high[...])
            level = level + dot(upper, lanes_low[...])
            resist = 1.0 / (1.0 + jnp.exp(-steepness * (level - threshold_level)))
            wanted = goal[rows, pl.ds(base, tile)].astype(jnp.float32)
            slope[rows] = (
                (2.0 * steepness * live) * (resist - wanted) * resist * (1.0 - resist)
            ).astype(bf)
            return carry

        lax.fori_loop(0, tile // 128, compare, 0)
        sloped[...] = dot(dot(over_rows_t[...], slope[...]).astype(bf), over_lanes[...]).astype(bf)

        def backward(k, carry):
            weight = sloped[...]
            cotangent = jnp.concatenate(
                [weight * fields[k, :points], weight * fields[k, points:]], axis=0)
            columns = dot(cotangent, grid_lanes_t[...]).astype(bf)
            columns = jnp.concatenate([columns[:points], columns[points:]], axis=1)
            top = dot(grid_rows[...], columns)
            tops = [top[:, : 2 * LANES], top[:, 2 * LANES :]]
            gather_adjoint(k, *tops, quads, acc)
            return carry

        lax.fori_loop(0, kernels, backward, 0, unroll=UNROLL)
        returned = dot(spectral_matrix(acc), outer_wide[...]).astype(bf)
        for first in (0, tile + AMBIT) + tuple(range(AMBIT, tile + AMBIT, AMBIT)):
            if first == AMBIT:
                for slot, dr, dc, copy in back:
                    if slot == now and dr:
                        only(dr, dc, copy.start)
            rows = pl.ds(first, AMBIT)
            piece = dot(outer_wide_t[rows], returned)
            edge = first in (0, tile + AMBIT)
            if now == 0:
                total[rows, pl.ds(0, extent)] = piece
                final = piece[:, :tile]
                if edge:
                    rim[rows, pl.ds(0, tile)] = final.astype(bf)
                else:
                    rim[rows, pl.ds(0, AMBIT)] = final[:, :AMBIT].astype(bf)
            else:
                both = total[rows, pl.ds(tile, extent - tile)] + piece[:, : extent - tile]
                total[rows, pl.ds(tile, extent - tile)] = both
                total[rows, pl.ds(extent, tile)] = piece[:, extent - tile :]
                if edge:
                    rim[rows, pl.ds(tile, extent - tile)] = both.astype(bf)
                    rim[rows, pl.ds(extent, tile)] = piece[:, extent - tile :].astype(bf)
                else:
                    rim[rows, pl.ds(width + AMBIT, AMBIT)] = piece[:, tile + AMBIT :].astype(bf)
        for slot, dr, dc, copy in back:
            if slot == now and not dr:
                only(dr, dc, copy.start)

    for now in range(2):
        for (slot, dr, dc, copy), entry in zip(back, rims(tile, width)):
            if slot != now:
                continue
            dst = entry[4]

            def add():
                copy.wait_recv()
                if dst[0] == "rows":
                    spot = (dst[1] * (tile - AMBIT), AMBIT, dst[2], dst[3])
                elif dst[0] == "cols":
                    spot = (0, tile, dst[1] * (width - AMBIT), AMBIT)
                else:
                    spot = (
                        dst[1] // 2 * (tile - AMBIT), AMBIT, dst[1] % 2 * (width - AMBIT), AMBIT)
                r, n, c, m = spot
                total[pl.ds(AMBIT + r, n), pl.ds(AMBIT + c, m)] += place(dst)[...].astype(jnp.float32)

            only(-dr, -dc, add)
    out[...] = total[pl.ds(AMBIT, tile), pl.ds(AMBIT, width)].astype(bf)
    for slot, dr, dc, copy in halo + back:
        only(dr, dc, copy.wait_send)


def body(grid, mask, target, live, pupils, weights):
    tile, width = mask.shape
    consts = tables(pupils.shape[2], tile)
    kernels = pupils.shape[1]
    bf, f32 = jnp.bfloat16, jnp.float32
    anywhere = pl.BlockSpec(memory_space=pl.ANY)
    smem = pl.BlockSpec(memory_space=pltpu.SMEM)
    extent = tile + 2 * AMBIT
    points, lanes = consts[7].shape[1], consts[1].shape[1]
    vmem = pl.BlockSpec(memory_space=pltpu.VMEM)
    gradient = pl.pallas_call(
        partial(kernel, grid),
        out_shape=jax.ShapeDtypeStruct(mask.shape, bf),
        in_specs=[smem, smem] + [anywhere] * (3 + len(consts)),
        out_specs=vmem,
        scratch_shapes=[pltpu.VMEM(t.shape, t.dtype) for t in consts]
        + [
            pltpu.VMEM((tile, width), f32),
            pltpu.VMEM((tile, width), bf),
            pltpu.VMEM(pupils.shape, f32),
            pltpu.VMEM((2, kernels, 2 * ROWS, 2 * LANES), f32),
            pltpu.VMEM((extent, width + 2 * AMBIT), bf),
            pltpu.VMEM((extent, width + 2 * AMBIT), f32),
            pltpu.VMEM((kernels, 2 * points, lanes), bf),
            pltpu.VMEM((points, lanes), f32),
            pltpu.VMEM((tile, tile), bf),
            pltpu.VMEM((points, lanes), bf),
            pltpu.VMEM((4, ROWS, LANES), f32),
            pltpu.VMEM((4, ROWS, LANES), f32),
            pltpu.VMEM(consts[0].shape[::-1], bf),
            pltpu.VMEM(consts[1].shape[::-1], bf),
            pltpu.VMEM(consts[5].shape[::-1], bf),
            pltpu.VMEM(consts[3].shape[::-1], bf),
            pltpu.VMEM((points, lanes), bf),
            pltpu.VMEM((points, lanes), bf),
            pltpu.VMEM((extent, width + 2 * AMBIT), bf),
            pltpu.VMEM((2, AMBIT, width), bf),
            pltpu.VMEM((2, tile, AMBIT), bf),
            pltpu.VMEM((4, AMBIT, AMBIT), bf),
            pltpu.SemaphoreType.DMA((5 + len(consts),)),
        ]
        + [pltpu.SemaphoreType.DMA((10,))] * 4,
        compiler_params=pltpu.CompilerParams(
            collective_id=0, has_side_effects=True, vmem_limit_bytes=VMEM_LIMIT
        ),
    )(live, weights, mask, target, pupils, *consts)
    return mask - step_rate * gradient.astype(f32)


def solution(mesh):
    return jax.shard_map(
        partial(body, (mesh.shape["row"], mesh.shape["col"])),
        mesh=mesh,
        in_specs=(P("row", "col"), P("row", "col"), P("row", "col"), P(), P()),
        out_specs=P("row", "col"),
        check_vma=False,
    )
```

```python
from functools import partial
import math

import jax
import jax.numpy as jnp
import numpy as np
from jax import lax
from jax.experimental import pallas as pl
from jax.experimental.pallas import tpu as pltpu
from jax.sharding import PartitionSpec as P

AMBIT = 128
ROWS = 80
LANES = 128

steepness = 4.0
threshold_level = 1.0
step_rate = 8.0

UNROLL = 6
VMEM_LIMIT = 60 * 1024 * 1024


def folded(count, pixels, offset, period, pad):
    half = count // 2
    frequency = np.arange(half + 1)
    place = np.arange(pixels) + offset
    phases = np.mod(frequency[:, None] * place[None, :], period).astype(np.float32)
    angles = phases * np.float32(2.0 * math.pi / period)
    factor = np.float32(1.0 / math.sqrt(period))
    table = np.zeros((2, pad, pixels), np.float32)
    table[0, : half + 1] = np.cos(angles) * factor
    table[1, : half + 1] = np.sin(angles) * factor
    return table.reshape(2 * pad, pixels)


def grid_table(count, points, period, pad):
    half = count // 2
    angles = np.arange(half + 1)[:, None] * np.arange(points)[None, :] * (2.0 * math.pi / points)
    table = np.zeros((2, pad, points))
    table[0, : half + 1] = np.cos(angles) / math.sqrt(period)
    table[1, : half + 1] = np.sin(angles) / math.sqrt(period)
    return table.reshape(2 * pad, points)


def between(count, points, pixels, offset, period):
    gap = np.arange(pixels)[:, None] + offset - np.arange(points)[None, :] * (period / points)
    gap = gap * (2.0 * math.pi / period)
    return (1.0 + 2.0 * sum(np.cos(m * gap) for m in range(1, count + 1))) / points


def halves(table):
    high = table.astype(jnp.bfloat16).astype(np.float64)
    return high, table - high


def tables(count, tile):
    extent = tile + 2 * AMBIT
    rows = -(-(2 * count + 1) // 16) * 16
    lanes = -(-(2 * count + 1) // 128) * 128
    grid_rows = grid_table(count, rows, extent, ROWS)
    grid_lanes = grid_table(count, lanes, extent, LANES)
    over_rows = between(count, rows, tile, AMBIT, extent)
    over_lanes = between(count, lanes, tile, AMBIT, extent)
    outer_wide = folded(count, extent, 0, extent, LANES)
    rows_high, rows_low = halves(over_rows)
    lanes_high, lanes_low = halves(over_lanes.T)
    return [
        jnp.asarray(t, jnp.bfloat16)
        for t in (
            outer_wide, grid_lanes, grid_rows.T, rows_high, rows_low, lanes_high, lanes_low,
            grid_rows,
        )
    ]


def dot(a, b):
    return jnp.dot(a, b, preferred_element_type=jnp.float32)


def split(value):
    upper = value.astype(jnp.bfloat16)
    return upper, (value - upper.astype(jnp.float32)).astype(jnp.bfloat16)


def times(ar, ai, br, bi):
    return ar * br - ai * bi, ar * bi + ai * br


def quarter(ref, part, k):
    return (
        ref[part, k, :ROWS, :LANES],
        ref[part, k, :ROWS, LANES:],
        ref[part, k, ROWS:, :LANES],
        ref[part, k, ROWS:, LANES:],
    )


def one_hot(shape, half, pad, along):
    place = lax.broadcasted_iota(jnp.int32, shape, along)
    source = lax.broadcasted_iota(jnp.int32, shape, 1 - along)
    above = place >= pad
    wanted = jnp.where(above, half + pad - place, half + place)
    hit = jnp.logical_and(source == wanted, place != pad)
    return jnp.where(hit, 1.0, 0.0).astype(jnp.bfloat16)


def fold_pupils(pupils, weights, quads):
    bf = jnp.bfloat16
    count = pupils.shape[3]
    left = one_hot((2 * ROWS, count), count // 2, ROWS, 0)
    right = one_hot((count, 2 * LANES), count // 2, LANES, 1)

    def one(k, carry):
        root = jnp.sqrt(jnp.full((1, pupils.shape[3]), weights[k], jnp.float32))
        for part in range(2):
            value = pupils[part, k] * root
            moved = [dot(left, dot(v, right).astype(bf)) for v in split(value)]
            quads[part, k] = moved[0] + moved[1]
        return carry

    lax.fori_loop(0, pupils.shape[1], one, 0)


def take_spectrum(window, outer_wide, outer_wide_t, spec):
    bf = jnp.bfloat16
    folds = jnp.concatenate([outer_wide[:ROWS], outer_wide[LANES : LANES + ROWS]], axis=0)
    partial_rows = dot(folds, window).astype(bf)
    blocks = dot(partial_rows, outer_wide_t[...])
    cc, cs = blocks[:ROWS, :LANES], blocks[:ROWS, LANES:]
    sc, ss = blocks[ROWS:, :LANES], blocks[ROWS:, LANES:]
    spec[0] = (cc - ss).astype(bf).astype(jnp.float32)
    spec[1] = -((cs + sc).astype(bf).astype(jnp.float32))
    spec[2] = (cc + ss).astype(bf).astype(jnp.float32)
    spec[3] = (cs - sc).astype(bf).astype(jnp.float32)


def amplitude_of(k, quads, spec):
    ar, br, cr, dr = quarter(quads, 0, k)
    ai, bi, ci, di = quarter(quads, 1, k)
    z1r, z1i, z2r, z2i = spec[0], spec[1], spec[2], spec[3]
    ppr, ppi = times(ar, ai, z1r, z1i)
    pnr, pni = times(br, bi, z2r, z2i)
    npr, npi = times(cr, ci, z2r, -z2i)
    nnr, nni = times(dr, di, z1r, -z1i)
    pr, pi, mr, mi = ppr + nnr, ppi + nni, ppr - nnr, ppi - nni
    qr, qi, nr, ni = pnr + npr, pni + npi, pnr - npr, pni - npi
    return jnp.concatenate(
        [
            jnp.concatenate([pr + qr, ni - mi], axis=1),
            jnp.concatenate([-(mi + ni), qr - pr], axis=1),
            jnp.concatenate([pi + qi, mr - nr], axis=1),
            jnp.concatenate([mr + nr, qi - pi], axis=1),
        ],
        axis=0,
    ).astype(jnp.bfloat16)


def gather_adjoint(k, re, im, quads, acc):
    ar, br, cr, dr = quarter(quads, 0, k)
    ai, bi, ci, di = quarter(quads, 1, k)
    ccr, csr, scr, ssr = re[:ROWS, :LANES], re[:ROWS, LANES:], re[ROWS:, :LANES], re[ROWS:, LANES:]
    cci, csi, sci, ssi = im[:ROWS, :LANES], im[:ROWS, LANES:], im[ROWS:, :LANES], im[ROWS:, LANES:]
    er, ei, fr, fi = ccr - ssr, cci - ssi, ccr + ssr, cci + ssi
    gr, gi, hr, hi = csr + scr, csi + sci, csr - scr, csi - sci
    ur, ui = times(ar, -ai, er + gi, ei - gr)
    vr, vi = times(dr, di, er - gi, -(ei + gr))
    acc[0] += ur + vr
    acc[1] += ui + vi
    ur, ui = times(br, -bi, fr - hi, fi + hr)
    vr, vi = times(cr, ci, fr + hi, hr - fi)
    acc[2] += ur + vr
    acc[3] += ui + vi


def spectral_matrix(acc):
    u1r, u1i, u2r, u2i = acc[0], acc[1], acc[2], acc[3]
    rest = jnp.zeros((LANES - ROWS, 2 * LANES), jnp.float32)
    return jnp.concatenate(
        [
            jnp.concatenate([u1r + u2r, u2i - u1i], axis=1),
            rest,
            jnp.concatenate([-(u1i + u2i), u2r - u1r], axis=1),
            rest,
        ],
        axis=0,
    ).astype(jnp.bfloat16)


def pieces(tile, width):
    low, high = tile + AMBIT, width + AMBIT
    split = tile + 2 * AMBIT
    rows = {-1: ((AMBIT, AMBIT), low), 0: ((AMBIT, tile), AMBIT), 1: ((tile, AMBIT), 0)}
    outs = []
    for slot in range(2):
        for dr in (-1, 1, 0):
            (first, count), place = rows[dr]
            if dr:
                c0, c1 = ((AMBIT, split), (split, high))[slot]
                outs.append((slot, dr, 0, (first, count, c0, c1 - c0), (place, count, c0, c1 - c0)))
            if slot == 0:
                outs.append((0, dr, 1, (first, count, width, AMBIT), (place, count, 0, AMBIT)))
            else:
                outs.append((1, dr, -1, (first, count, AMBIT, AMBIT), (place, count, high, AMBIT)))
    return outs


def rims(tile, width):
    low, high = tile + AMBIT, width + AMBIT
    cut = tile - AMBIT
    outs = []
    for slot in range(2):
        for dr in (-1, 1, 0):
            first, count = ((AMBIT, tile), (low, AMBIT), (0, AMBIT))[dr]
            side = 1 if dr < 0 else 0
            if dr:
                c0, c1 = ((AMBIT, tile), (tile, high))[slot]
                outs.append((slot, dr, 0, (first, count, c0, c1 - c0), ("rows", side, c0 - AMBIT, c1 - c0)))
            dc, c0, other = ((-1, 0, 1), (1, high, 0))[slot]
            if dr:
                outs.append((slot, dr, dc, (first, count, c0, AMBIT), ("corner", 2 * side + other)))
            else:
                outs.append((slot, 0, dc, (first, count, c0, AMBIT), ("cols", other)))
    return outs


def window(ref, place):
    row, rows, col, cols = place
    return ref.at[pl.ds(row, rows), pl.ds(col, cols)]


def kernel(
    grid, live_ref, weight_ref, mask_hbm, goal_hbm, pupil_hbm, *refs,
):
    tables_hbm, refs = refs[:8], refs[8:]
    out = refs[0]
    held, refs = refs[1:9], refs[9:]
    (
        mask, goal, pupils, quads, ext, total, fields, intensity, slope, sloped, spec, acc,
        outer_wide_t, grid_lanes_t, over_lanes, over_rows_t, high, low, rim, got_rows, got_cols, got_corner, in_sem, halo_send, halo_recv, rim_send, rim_recv,
    ) = refs
    (
        outer_wide, grid_lanes, grid_rows_t, rows_high, rows_low, lanes_high, lanes_low, grid_rows,
    ) = held
    bf = jnp.bfloat16
    tile, width = mask.shape
    extent = tile + 2 * AMBIT
    kernels = pupils.shape[1]
    row, col = lax.axis_index("row"), lax.axis_index("col")
    last_row, last_col = grid[0] - 1, grid[1] - 1

    def there(dr, dc):
        ok = jnp.bool_(True)
        if dr:
            ok = row > 0 if dr < 0 else row < last_row
        if dc:
            side = col > 0 if dc < 0 else col < last_col
            ok = jnp.logical_and(ok, side) if dr else side
        return ok

    def only(dr, dc, act):
        pl.when(there(dr, dc))(act)

    cuts = ((0, AMBIT), (tile - AMBIT, AMBIT), (AMBIT, tile - 2 * AMBIT))
    loads = [
        pltpu.make_async_copy(mask_hbm.at[pl.ds(a, n)], mask.at[pl.ds(a, n)], in_sem.at[i])
        for i, (a, n) in enumerate(cuts)
    ]
    loads.append(pltpu.make_async_copy(pupil_hbm, pupils, in_sem.at[3]))
    first_table = len(loads)
    for source, target in zip(tables_hbm, held):
        loads.append(pltpu.make_async_copy(source, target, in_sem.at[len(loads)]))
    goal_load = len(loads)
    loads.append(pltpu.make_async_copy(goal_hbm, goal, in_sem.at[goal_load]))
    for load in loads[:3]:
        load.start()

    barrier = pltpu.get_barrier_semaphore()
    around = [(dr, dc) for dr in (-1, 0, 1) for dc in (-1, 0, 1) if dr or dc]
    for dr, dc in around:
        only(dr, dc, lambda: pl.semaphore_signal(
            barrier, inc=1, device_id=(row + dr, col + dc), device_id_type=pl.DeviceIdType.MESH))
    def take(i):
        start, count = cuts[i]
        loads[i].wait()
        ext[pl.ds(AMBIT + start, count), pl.ds(AMBIT, width)] = mask[pl.ds(start, count)].astype(bf)

    take(0)
    take(1)
    for load in loads[3:]:
        load.start()
    tall = 3 - (row == 0).astype(jnp.int32) - (row == last_row).astype(jnp.int32)
    broad = 3 - (col == 0).astype(jnp.int32) - (col == last_col).astype(jnp.int32)
    pl.semaphore_wait(barrier, tall * broad - 1)

    def copies(table, source, target, send, recv):
        outs = []
        for i, (slot, dr, dc, src, dst) in enumerate(table):
            outs.append((slot, dr, dc, pltpu.make_async_remote_copy(
                src_ref=window(source, src), dst_ref=target(dst), send_sem=send.at[i],
                recv_sem=recv.at[i], device_id=(row + dr, col + dc),
                device_id_type=pl.DeviceIdType.MESH)))
        return outs

    def place(dst):
        if dst[0] == "rows":
            return got_rows.at[dst[1], :, pl.ds(dst[2], dst[3])]
        return got_cols.at[dst[1]] if dst[0] == "cols" else got_corner.at[dst[1]]

    halo = copies(pieces(tile, width), ext, lambda dst: window(ext, dst), halo_send, halo_recv)
    back = copies(rims(tile, width), rim, place, rim_send, rim_recv)
    for slot, dr, dc, copy in halo:
        if dr:
            only(dr, dc, copy.start)
    take(2)
    for slot, dr, dc, copy in halo:
        if not dr:
            only(dr, dc, copy.start)
    for slot, dr, dc, src, dst in pieces(tile, width):

        def clear():
            ext[pl.ds(dst[0], dst[1]), pl.ds(dst[2], dst[3])] = jnp.zeros((dst[1], dst[3]), bf)

        pl.when(jnp.logical_not(there(-dr, -dc)))(clear)

    loads[3].wait()
    fold_pupils(pupils, weight_ref, quads)
    for load in loads[first_table:]:
        load.wait()
    points = grid_rows.shape[1]
    outer_wide_t[...] = outer_wide[...].T
    grid_lanes_t[...] = grid_lanes[...].T
    over_lanes[...] = lanes_high[...].T
    over_rows_t[...] = rows_high[...].T

    for now in range(2):
        for slot, dr, dc, copy in halo:
            if slot == now:
                only(-dr, -dc, copy.wait_recv)
        base = now * tile
        take_spectrum(ext[:, pl.ds(base, extent)], outer_wide, outer_wide_t, spec)
        intensity[...] = jnp.zeros_like(intensity)
        acc[...] = jnp.zeros_like(acc)

        def forward(k, carry):
            section = dot(amplitude_of(k, quads, spec), grid_lanes[...]).astype(bf)
            both = jnp.concatenate([section[: 2 * ROWS], section[2 * ROWS :]], axis=1)
            field = dot(grid_rows_t[...], both)
            lanes = grid_lanes.shape[1]
            field_re, field_im = field[:, :lanes], field[:, lanes:]
            intensity[...] += field_re * field_re + field_im * field_im
            fields[k, :points] = field_re.astype(bf)
            fields[k, points:] = field_im.astype(bf)
            return carry

        lax.fori_loop(0, kernels, forward, 0, unroll=UNROLL)
        high[...], low[...] = split(intensity[...])
        live = live_ref[0, now].astype(jnp.float32)
        def compare(part, carry):
            rows = pl.ds(pl.multiple_of(part * 128, 128), 128)
            level = dot(rows_high[rows], high[...]) + dot(rows_high[rows], low[...])
            level = level + dot(rows_low[rows], high[...])
            upper, lower = split(level)
            level = dot(upper, lanes_high[...]) + dot(lower, lanes_high[...])
            level = level + dot(upper, lanes_low[...])
            resist = 1.0 / (1.0 + jnp.exp(-steepness * (level - threshold_level)))
            wanted = goal[rows, pl.ds(base, tile)].astype(jnp.float32)
            slope[rows] = (
                (2.0 * steepness * live) * (resist - wanted) * resist * (1.0 - resist)
            ).astype(bf)
            return carry

        lax.fori_loop(0, tile // 128, compare, 0)
        sloped[...] = dot(dot(over_rows_t[...], slope[...]).astype(bf), over_lanes[...]).astype(bf)

        def backward(k, carry):
            weight = sloped[...]
            cotangent = jnp.concatenate(
                [weight * fields[k, :points], weight * fields[k, points:]], axis=0)
            columns = dot(cotangent, grid_lanes_t[...]).astype(bf)
            columns = jnp.concatenate([columns[:points], columns[points:]], axis=1)
            top = dot(grid_rows[...], columns)
            tops = [top[:, : 2 * LANES], top[:, 2 * LANES :]]
            gather_adjoint(k, *tops, quads, acc)
            return carry

        lax.fori_loop(0, kernels, backward, 0, unroll=UNROLL)
        returned = dot(spectral_matrix(acc), outer_wide[...]).astype(bf)
        for first in (0, tile + AMBIT) + tuple(range(AMBIT, tile + AMBIT, AMBIT)):
            if first == AMBIT:
                for slot, dr, dc, copy in back:
                    if slot == now and dr:
                        only(dr, dc, copy.start)
            rows = pl.ds(first, AMBIT)
            piece = dot(outer_wide_t[rows], returned)
            edge = first in (0, tile + AMBIT)
            if now == 0:
                total[rows, pl.ds(0, extent)] = piece
                final = piece[:, :tile]
                if edge:
                    rim[rows, pl.ds(0, tile)] = final.astype(bf)
                else:
                    rim[rows, pl.ds(0, AMBIT)] = final[:, :AMBIT].astype(bf)
            else:
                both = total[rows, pl.ds(tile, extent - tile)] + piece[:, : extent - tile]
                total[rows, pl.ds(tile, extent - tile)] = both
                total[rows, pl.ds(extent, tile)] = piece[:, extent - tile :]
                if edge:
                    rim[rows, pl.ds(tile, extent - tile)] = both.astype(bf)
                    rim[rows, pl.ds(extent, tile)] = piece[:, extent - tile :].astype(bf)
                else:
                    rim[rows, pl.ds(width + AMBIT, AMBIT)] = piece[:, tile + AMBIT :].astype(bf)
        for slot, dr, dc, copy in back:
            if slot == now and not dr:
                only(dr, dc, copy.start)

    def leave(r, n, c, m):
        out[pl.ds(r, n), pl.ds(c, m)] = total[pl.ds(AMBIT + r, n), pl.ds(AMBIT + c, m)].astype(bf)

    inner_rows = tile - 2 * AMBIT
    leave(AMBIT, inner_rows, AMBIT, width - 2 * AMBIT)
    for now in range(2):
        for (slot, dr, dc, copy), entry in zip(back, rims(tile, width)):
            if slot != now:
                continue
            dst = entry[4]

            def add():
                copy.wait_recv()
                if dst[0] == "rows":
                    spot = (dst[1] * (tile - AMBIT), AMBIT, dst[2], dst[3])
                elif dst[0] == "cols":
                    spot = (0, tile, dst[1] * (width - AMBIT), AMBIT)
                else:
                    spot = (
                        dst[1] // 2 * (tile - AMBIT), AMBIT, dst[1] % 2 * (width - AMBIT), AMBIT)
                r, n, c, m = spot
                total[pl.ds(AMBIT + r, n), pl.ds(AMBIT + c, m)] += place(dst)[...].astype(jnp.float32)

            only(-dr, -dc, add)
    leave(0, AMBIT, 0, width)
    leave(tile - AMBIT, AMBIT, 0, width)
    leave(AMBIT, inner_rows, 0, AMBIT)
    leave(AMBIT, inner_rows, width - AMBIT, AMBIT)
    for slot, dr, dc, copy in halo + back:
        only(dr, dc, copy.wait_send)


def body(grid, mask, target, live, pupils, weights):
    tile, width = mask.shape
    consts = tables(pupils.shape[2], tile)
    kernels = pupils.shape[1]
    bf, f32 = jnp.bfloat16, jnp.float32
    anywhere = pl.BlockSpec(memory_space=pl.ANY)
    smem = pl.BlockSpec(memory_space=pltpu.SMEM)
    extent = tile + 2 * AMBIT
    points, lanes = consts[7].shape[1], consts[1].shape[1]
    vmem = pl.BlockSpec(memory_space=pltpu.VMEM)
    gradient = pl.pallas_call(
        partial(kernel, grid),
        out_shape=jax.ShapeDtypeStruct(mask.shape, bf),
        in_specs=[smem, smem] + [anywhere] * (3 + len(consts)),
        out_specs=vmem,
        scratch_shapes=[pltpu.VMEM(t.shape, t.dtype) for t in consts]
        + [
            pltpu.VMEM((tile, width), f32),
            pltpu.VMEM((tile, width), bf),
            pltpu.VMEM(pupils.shape, f32),
            pltpu.VMEM((2, kernels, 2 * ROWS, 2 * LANES), f32),
            pltpu.VMEM((extent, width + 2 * AMBIT), bf),
            pltpu.VMEM((extent, width + 2 * AMBIT), f32),
            pltpu.VMEM((kernels, 2 * points, lanes), bf),
            pltpu.VMEM((points, lanes), f32),
            pltpu.VMEM((tile, tile), bf),
            pltpu.VMEM((points, lanes), bf),
            pltpu.VMEM((4, ROWS, LANES), f32),
            pltpu.VMEM((4, ROWS, LANES), f32),
            pltpu.VMEM(consts[0].shape[::-1], bf),
            pltpu.VMEM(consts[1].shape[::-1], bf),
            pltpu.VMEM(consts[5].shape[::-1], bf),
            pltpu.VMEM(consts[3].shape[::-1], bf),
            pltpu.VMEM((points, lanes), bf),
            pltpu.VMEM((points, lanes), bf),
            pltpu.VMEM((extent, width + 2 * AMBIT), bf),
            pltpu.VMEM((2, AMBIT, width), bf),
            pltpu.VMEM((2, tile, AMBIT), bf),
            pltpu.VMEM((4, AMBIT, AMBIT), bf),
            pltpu.SemaphoreType.DMA((5 + len(consts),)),
        ]
        + [pltpu.SemaphoreType.DMA((10,))] * 4,
        compiler_params=pltpu.CompilerParams(
            collective_id=0, has_side_effects=True, vmem_limit_bytes=VMEM_LIMIT
        ),
    )(live, weights, mask, target, pupils, *consts)
    return mask - step_rate * gradient.astype(f32)


def solution(mesh):
    return jax.shard_map(
        partial(body, (mesh.shape["row"], mesh.shape["col"])),
        mesh=mesh,
        in_specs=(P("row", "col"), P("row", "col"), P("row", "col"), P(), P()),
        out_specs=P("row", "col"),
        check_vma=False,
    )
```

```python
from functools import partial
import math

import jax
import jax.numpy as jnp
import numpy as np
from jax import lax
from jax.experimental import pallas as pl
from jax.experimental.pallas import tpu as pltpu
from jax.sharding import PartitionSpec as P

AMBIT = 128
ROWS = 80
LANES = 128

steepness = 4.0
threshold_level = 1.0
step_rate = 8.0

UNROLL = 6
VMEM_LIMIT = 60 * 1024 * 1024


def folded(count, pixels, offset, period, pad):
    half = count // 2
    frequency = np.arange(half + 1)
    place = np.arange(pixels) + offset
    phases = np.mod(frequency[:, None] * place[None, :], period).astype(np.float32)
    angles = phases * np.float32(2.0 * math.pi / period)
    factor = np.float32(1.0 / math.sqrt(period))
    table = np.zeros((2, pad, pixels), np.float32)
    table[0, : half + 1] = np.cos(angles) * factor
    table[1, : half + 1] = np.sin(angles) * factor
    return table.reshape(2 * pad, pixels)


def grid_table(count, points, period, pad):
    half = count // 2
    angles = np.arange(half + 1)[:, None] * np.arange(points)[None, :] * (2.0 * math.pi / points)
    table = np.zeros((2, pad, points))
    table[0, : half + 1] = np.cos(angles) / math.sqrt(period)
    table[1, : half + 1] = np.sin(angles) / math.sqrt(period)
    return table.reshape(2 * pad, points)


def between(count, points, pixels, offset, period):
    gap = np.arange(pixels)[:, None] + offset - np.arange(points)[None, :] * (period / points)
    gap = gap * (2.0 * math.pi / period)
    return (1.0 + 2.0 * sum(np.cos(m * gap) for m in range(1, count + 1))) / points


def halves(table):
    high = table.astype(jnp.bfloat16).astype(np.float64)
    return high, table - high


def tables(count, tile):
    extent = tile + 2 * AMBIT
    rows = -(-(2 * count + 1) // 16) * 16
    lanes = -(-(2 * count + 1) // 128) * 128
    grid_rows = grid_table(count, rows, extent, ROWS)
    grid_lanes = grid_table(count, lanes, extent, LANES)
    over_rows = between(count, rows, tile, AMBIT, extent)
    over_lanes = between(count, lanes, tile, AMBIT, extent)
    outer_wide = folded(count, extent, 0, extent, LANES)
    rows_high, rows_low = halves(over_rows)
    lanes_high, lanes_low = halves(over_lanes.T)
    return [
        jnp.asarray(t, jnp.bfloat16)
        for t in (
            outer_wide, grid_lanes, grid_rows.T, rows_high, rows_low, lanes_high, lanes_low,
            grid_rows,
        )
    ]


def dot(a, b):
    return jnp.dot(a, b, preferred_element_type=jnp.float32)


def split(value):
    upper = value.astype(jnp.bfloat16)
    return upper, (value - upper.astype(jnp.float32)).astype(jnp.bfloat16)


def times(ar, ai, br, bi):
    return ar * br - ai * bi, ar * bi + ai * br


def quarter(ref, part, k):
    return (
        ref[part, k, :ROWS, :LANES],
        ref[part, k, :ROWS, LANES:],
        ref[part, k, ROWS:, :LANES],
        ref[part, k, ROWS:, LANES:],
    )


def one_hot(shape, half, pad, along):
    place = lax.broadcasted_iota(jnp.int32, shape, along)
    source = lax.broadcasted_iota(jnp.int32, shape, 1 - along)
    above = place >= pad
    wanted = jnp.where(above, half + pad - place, half + place)
    hit = jnp.logical_and(source == wanted, place != pad)
    return jnp.where(hit, 1.0, 0.0).astype(jnp.bfloat16)


def fold_pupils(pupils, weights, quads):
    bf = jnp.bfloat16
    count = pupils.shape[3]
    left = one_hot((2 * ROWS, count), count // 2, ROWS, 0)
    right = one_hot((count, 2 * LANES), count // 2, LANES, 1)

    def one(k, carry):
        root = jnp.sqrt(jnp.full((1, pupils.shape[3]), weights[k], jnp.float32))
        for part in range(2):
            value = pupils[part, k] * root
            moved = [dot(left, dot(v, right).astype(bf)) for v in split(value)]
            quads[part, k] = moved[0] + moved[1]
        return carry

    lax.fori_loop(0, pupils.shape[1], one, 0)


def take_spectrum(window, outer_wide, outer_wide_t, spec):
    bf = jnp.bfloat16
    folds = jnp.concatenate([outer_wide[:ROWS], outer_wide[LANES : LANES + ROWS]], axis=0)
    partial_rows = dot(folds, window).astype(bf)
    blocks = dot(partial_rows, outer_wide_t[...])
    cc, cs = blocks[:ROWS, :LANES], blocks[:ROWS, LANES:]
    sc, ss = blocks[ROWS:, :LANES], blocks[ROWS:, LANES:]
    spec[0] = (cc - ss).astype(bf).astype(jnp.float32)
    spec[1] = -((cs + sc).astype(bf).astype(jnp.float32))
    spec[2] = (cc + ss).astype(bf).astype(jnp.float32)
    spec[3] = (cs - sc).astype(bf).astype(jnp.float32)


def amplitude_of(k, quads, spec):
    ar, br, cr, dr = quarter(quads, 0, k)
    ai, bi, ci, di = quarter(quads, 1, k)
    z1r, z1i, z2r, z2i = spec[0], spec[1], spec[2], spec[3]
    ppr, ppi = times(ar, ai, z1r, z1i)
    pnr, pni = times(br, bi, z2r, z2i)
    npr, npi = times(cr, ci, z2r, -z2i)
    nnr, nni = times(dr, di, z1r, -z1i)
    pr, pi, mr, mi = ppr + nnr, ppi + nni, ppr - nnr, ppi - nni
    qr, qi, nr, ni = pnr + npr, pni + npi, pnr - npr, pni - npi
    return jnp.concatenate(
        [
            jnp.concatenate([pr + qr, ni - mi], axis=1),
            jnp.concatenate([-(mi + ni), qr - pr], axis=1),
            jnp.concatenate([pi + qi, mr - nr], axis=1),
            jnp.concatenate([mr + nr, qi - pi], axis=1),
        ],
        axis=0,
    ).astype(jnp.bfloat16)


def gather_adjoint(k, re, im, quads, acc):
    ar, br, cr, dr = quarter(quads, 0, k)
    ai, bi, ci, di = quarter(quads, 1, k)
    ccr, csr, scr, ssr = re[:ROWS, :LANES], re[:ROWS, LANES:], re[ROWS:, :LANES], re[ROWS:, LANES:]
    cci, csi, sci, ssi = im[:ROWS, :LANES], im[:ROWS, LANES:], im[ROWS:, :LANES], im[ROWS:, LANES:]
    er, ei, fr, fi = ccr - ssr, cci - ssi, ccr + ssr, cci + ssi
    gr, gi, hr, hi = csr + scr, csi + sci, csr - scr, csi - sci
    ur, ui = times(ar, -ai, er + gi, ei - gr)
    vr, vi = times(dr, di, er - gi, -(ei + gr))
    acc[0] += ur + vr
    acc[1] += ui + vi
    ur, ui = times(br, -bi, fr - hi, fi + hr)
    vr, vi = times(cr, ci, fr + hi, hr - fi)
    acc[2] += ur + vr
    acc[3] += ui + vi


def spectral_matrix(acc):
    u1r, u1i, u2r, u2i = acc[0], acc[1], acc[2], acc[3]
    rest = jnp.zeros((LANES - ROWS, 2 * LANES), jnp.float32)
    return jnp.concatenate(
        [
            jnp.concatenate([u1r + u2r, u2i - u1i], axis=1),
            rest,
            jnp.concatenate([-(u1i + u2i), u2r - u1r], axis=1),
            rest,
        ],
        axis=0,
    ).astype(jnp.bfloat16)


def pieces(tile, width):
    low, high = tile + AMBIT, width + AMBIT
    split = tile + 2 * AMBIT
    rows = {-1: ((AMBIT, AMBIT), low), 0: ((AMBIT, tile), AMBIT), 1: ((tile, AMBIT), 0)}
    outs = []
    for slot in range(2):
        for dr in (-1, 1, 0):
            (first, count), place = rows[dr]
            if dr:
                c0, c1 = ((AMBIT, split), (split, high))[slot]
                outs.append((slot, dr, 0, (first, count, c0, c1 - c0), (place, count, c0, c1 - c0)))
            if slot == 0:
                outs.append((0, dr, 1, (first, count, width, AMBIT), (place, count, 0, AMBIT)))
            else:
                outs.append((1, dr, -1, (first, count, AMBIT, AMBIT), (place, count, high, AMBIT)))
    return outs


def rims(tile, width):
    low, high = tile + AMBIT, width + AMBIT
    cut = tile - AMBIT
    outs = []
    for slot in range(2):
        for dr in (-1, 1, 0):
            first, count = ((AMBIT, tile), (low, AMBIT), (0, AMBIT))[dr]
            side = 1 if dr < 0 else 0
            if dr:
                c0, c1 = ((AMBIT, tile), (tile, high))[slot]
                outs.append((slot, dr, 0, (first, count, c0, c1 - c0), ("rows", side, c0 - AMBIT, c1 - c0)))
            dc, c0, other = ((-1, 0, 1), (1, high, 0))[slot]
            if dr:
                outs.append((slot, dr, dc, (first, count, c0, AMBIT), ("corner", 2 * side + other)))
            else:
                outs.append((slot, 0, dc, (first, count, c0, AMBIT), ("cols", other)))
    return outs


def window(ref, place):
    row, rows, col, cols = place
    return ref.at[pl.ds(row, rows), pl.ds(col, cols)]


def kernel(
    grid, live_ref, weight_ref, mask_hbm, goal_hbm, pupil_hbm, *refs,
):
    tables_hbm, refs = refs[:8], refs[8:]
    out = refs[0]
    held, refs = refs[1:9], refs[9:]
    (
        mask, goal, pupils, quads, ext, total, fields, intensity, slope, sloped, spec, acc,
        outer_wide_t, grid_lanes_t, over_lanes, over_rows_t, high, low, rim, got_rows, got_cols, got_corner, in_sem, halo_send, halo_recv, rim_send, rim_recv,
    ) = refs
    (
        outer_wide, grid_lanes, grid_rows_t, rows_high, rows_low, lanes_high, lanes_low, grid_rows,
    ) = held
    bf = jnp.bfloat16
    tile, width = mask.shape
    extent = tile + 2 * AMBIT
    kernels = pupils.shape[1]
    row, col = lax.axis_index("row"), lax.axis_index("col")
    last_row, last_col = grid[0] - 1, grid[1] - 1

    def there(dr, dc):
        ok = jnp.bool_(True)
        if dr:
            ok = row > 0 if dr < 0 else row < last_row
        if dc:
            side = col > 0 if dc < 0 else col < last_col
            ok = jnp.logical_and(ok, side) if dr else side
        return ok

    def only(dr, dc, act):
        pl.when(there(dr, dc))(act)

    cuts = ((0, AMBIT), (tile - AMBIT, AMBIT), (AMBIT, tile - 2 * AMBIT))
    loads = [
        pltpu.make_async_copy(mask_hbm.at[pl.ds(a, n)], mask.at[pl.ds(a, n)], in_sem.at[i])
        for i, (a, n) in enumerate(cuts)
    ]
    loads.append(pltpu.make_async_copy(pupil_hbm, pupils, in_sem.at[3]))
    first_table = len(loads)
    for source, target in zip(tables_hbm, held):
        loads.append(pltpu.make_async_copy(source, target, in_sem.at[len(loads)]))
    goal_load = len(loads)
    loads.append(pltpu.make_async_copy(goal_hbm, goal, in_sem.at[goal_load]))
    for load in loads[:4]:
        load.start()

    barrier = pltpu.get_barrier_semaphore()
    around = [(dr, dc) for dr in (-1, 0, 1) for dc in (-1, 0, 1) if dr or dc]
    for dr, dc in around:
        only(dr, dc, lambda: pl.semaphore_signal(
            barrier, inc=1, device_id=(row + dr, col + dc), device_id_type=pl.DeviceIdType.MESH))
    def take(i):
        start, count = cuts[i]
        loads[i].wait()
        ext[pl.ds(AMBIT + start, count), pl.ds(AMBIT, width)] = mask[pl.ds(start, count)].astype(bf)

    take(0)
    take(1)
    for load in loads[4:]:
        load.start()
    tall = 3 - (row == 0).astype(jnp.int32) - (row == last_row).astype(jnp.int32)
    broad = 3 - (col == 0).astype(jnp.int32) - (col == last_col).astype(jnp.int32)
    pl.semaphore_wait(barrier, tall * broad - 1)

    def copies(table, source, target, send, recv):
        outs = []
        for i, (slot, dr, dc, src, dst) in enumerate(table):
            outs.append((slot, dr, dc, pltpu.make_async_remote_copy(
                src_ref=window(source, src), dst_ref=target(dst), send_sem=send.at[i],
                recv_sem=recv.at[i], device_id=(row + dr, col + dc),
                device_id_type=pl.DeviceIdType.MESH)))
        return outs

    def place(dst):
        if dst[0] == "rows":
            return got_rows.at[dst[1], :, pl.ds(dst[2], dst[3])]
        return got_cols.at[dst[1]] if dst[0] == "cols" else got_corner.at[dst[1]]

    halo = copies(pieces(tile, width), ext, lambda dst: window(ext, dst), halo_send, halo_recv)
    back = copies(rims(tile, width), rim, place, rim_send, rim_recv)
    for slot, dr, dc, copy in halo:
        if dr:
            only(dr, dc, copy.start)
    take(2)
    for slot, dr, dc, copy in halo:
        if not dr:
            only(dr, dc, copy.start)
    for slot, dr, dc, src, dst in pieces(tile, width):

        def clear():
            ext[pl.ds(dst[0], dst[1]), pl.ds(dst[2], dst[3])] = jnp.zeros((dst[1], dst[3]), bf)

        pl.when(jnp.logical_not(there(-dr, -dc)))(clear)

    loads[3].wait()
    fold_pupils(pupils, weight_ref, quads)
    for load in loads[first_table:]:
        load.wait()
    points = grid_rows.shape[1]
    outer_wide_t[...] = outer_wide[...].T
    grid_lanes_t[...] = grid_lanes[...].T
    over_lanes[...] = lanes_high[...].T
    over_rows_t[...] = rows_high[...].T

    for now in range(2):
        for slot, dr, dc, copy in halo:
            if slot == now:
                only(-dr, -dc, copy.wait_recv)
        base = now * tile
        take_spectrum(ext[:, pl.ds(base, extent)], outer_wide, outer_wide_t, spec)
        intensity[...] = jnp.zeros_like(intensity)
        acc[...] = jnp.zeros_like(acc)

        def forward(k, carry):
            section = dot(amplitude_of(k, quads, spec), grid_lanes[...]).astype(bf)
            both = jnp.concatenate([section[: 2 * ROWS], section[2 * ROWS :]], axis=1)
            field = dot(grid_rows_t[...], both)
            lanes = grid_lanes.shape[1]
            field_re, field_im = field[:, :lanes], field[:, lanes:]
            intensity[...] += field_re * field_re + field_im * field_im
            fields[k, :points] = field_re.astype(bf)
            fields[k, points:] = field_im.astype(bf)
            return carry

        lax.fori_loop(0, kernels, forward, 0, unroll=UNROLL)
        high[...], low[...] = split(intensity[...])
        live = live_ref[0, now].astype(jnp.float32)
        def compare(part, carry):
            rows = pl.ds(pl.multiple_of(part * 128, 128), 128)
            level = dot(rows_high[rows], high[...]) + dot(rows_high[rows], low[...])
            level = level + dot(rows_low[rows], high[...])
            upper, lower = split(level)
            level = dot(upper, lanes_high[...]) + dot(lower, lanes_high[...])
            level = level + dot(upper, lanes_low[...])
            resist = 1.0 / (1.0 + jnp.exp(-steepness * (level - threshold_level)))
            wanted = goal[rows, pl.ds(base, tile)].astype(jnp.float32)
            slope[rows] = (
                (2.0 * steepness * live) * (resist - wanted) * resist * (1.0 - resist)
            ).astype(bf)
            return carry

        lax.fori_loop(0, tile // 128, compare, 0)
        sloped[...] = dot(dot(over_rows_t[...], slope[...]).astype(bf), over_lanes[...]).astype(bf)

        def backward(k, carry):
            weight = sloped[...]
            cotangent = jnp.concatenate(
                [weight * fields[k, :points], weight * fields[k, points:]], axis=0)
            columns = dot(cotangent, grid_lanes_t[...]).astype(bf)
            columns = jnp.concatenate([columns[:points], columns[points:]], axis=1)
            top = dot(grid_rows[...], columns)
            tops = [top[:, : 2 * LANES], top[:, 2 * LANES :]]
            gather_adjoint(k, *tops, quads, acc)
            return carry

        lax.fori_loop(0, kernels, backward, 0, unroll=UNROLL)
        returned = dot(spectral_matrix(acc), outer_wide[...]).astype(bf)
        for first in (0, tile + AMBIT) + tuple(range(AMBIT, tile + AMBIT, AMBIT)):
            if first == AMBIT:
                for slot, dr, dc, copy in back:
                    if slot == now and dr:
                        only(dr, dc, copy.start)
            rows = pl.ds(first, AMBIT)
            piece = dot(outer_wide_t[rows], returned)
            edge = first in (0, tile + AMBIT)
            if now == 0:
                total[rows, pl.ds(0, extent)] = piece
                final = piece[:, :tile]
                if edge:
                    rim[rows, pl.ds(0, tile)] = final.astype(bf)
                else:
                    rim[rows, pl.ds(0, AMBIT)] = final[:, :AMBIT].astype(bf)
            else:
                both = total[rows, pl.ds(tile, extent - tile)] + piece[:, : extent - tile]
                total[rows, pl.ds(tile, extent - tile)] = both
                total[rows, pl.ds(extent, tile)] = piece[:, extent - tile :]
                if edge:
                    rim[rows, pl.ds(tile, extent - tile)] = both.astype(bf)
                    rim[rows, pl.ds(extent, tile)] = piece[:, extent - tile :].astype(bf)
                else:
                    rim[rows, pl.ds(width + AMBIT, AMBIT)] = piece[:, tile + AMBIT :].astype(bf)
        for slot, dr, dc, copy in back:
            if slot == now and not dr:
                only(dr, dc, copy.start)

    def leave(r, n, c, m):
        out[pl.ds(r, n), pl.ds(c, m)] = total[pl.ds(AMBIT + r, n), pl.ds(AMBIT + c, m)].astype(bf)

    inner_rows = tile - 2 * AMBIT
    leave(AMBIT, inner_rows, AMBIT, width - 2 * AMBIT)
    for now in range(2):
        for (slot, dr, dc, copy), entry in zip(back, rims(tile, width)):
            if slot != now:
                continue
            dst = entry[4]

            def add():
                copy.wait_recv()
                if dst[0] == "rows":
                    spot = (dst[1] * (tile - AMBIT), AMBIT, dst[2], dst[3])
                elif dst[0] == "cols":
                    spot = (0, tile, dst[1] * (width - AMBIT), AMBIT)
                else:
                    spot = (
                        dst[1] // 2 * (tile - AMBIT), AMBIT, dst[1] % 2 * (width - AMBIT), AMBIT)
                r, n, c, m = spot
                total[pl.ds(AMBIT + r, n), pl.ds(AMBIT + c, m)] += place(dst)[...].astype(jnp.float32)

            only(-dr, -dc, add)
    leave(0, AMBIT, 0, width)
    leave(tile - AMBIT, AMBIT, 0, width)
    leave(AMBIT, inner_rows, 0, AMBIT)
    leave(AMBIT, inner_rows, width - AMBIT, AMBIT)
    for slot, dr, dc, copy in halo + back:
        only(dr, dc, copy.wait_send)


def body(grid, mask, target, live, pupils, weights):
    tile, width = mask.shape
    consts = tables(pupils.shape[2], tile)
    kernels = pupils.shape[1]
    bf, f32 = jnp.bfloat16, jnp.float32
    anywhere = pl.BlockSpec(memory_space=pl.ANY)
    smem = pl.BlockSpec(memory_space=pltpu.SMEM)
    extent = tile + 2 * AMBIT
    points, lanes = consts[7].shape[1], consts[1].shape[1]
    vmem = pl.BlockSpec(memory_space=pltpu.VMEM)
    gradient = pl.pallas_call(
        partial(kernel, grid),
        out_shape=jax.ShapeDtypeStruct(mask.shape, bf),
        in_specs=[smem, smem] + [anywhere] * (3 + len(consts)),
        out_specs=vmem,
        scratch_shapes=[pltpu.VMEM(t.shape, t.dtype) for t in consts]
        + [
            pltpu.VMEM((tile, width), f32),
            pltpu.VMEM((tile, width), bf),
            pltpu.VMEM(pupils.shape, f32),
            pltpu.VMEM((2, kernels, 2 * ROWS, 2 * LANES), f32),
            pltpu.VMEM((extent, width + 2 * AMBIT), bf),
            pltpu.VMEM((extent, width + 2 * AMBIT), f32),
            pltpu.VMEM((kernels, 2 * points, lanes), bf),
            pltpu.VMEM((points, lanes), f32),
            pltpu.VMEM((tile, tile), bf),
            pltpu.VMEM((points, lanes), bf),
            pltpu.VMEM((4, ROWS, LANES), f32),
            pltpu.VMEM((4, ROWS, LANES), f32),
            pltpu.VMEM(consts[0].shape[::-1], bf),
            pltpu.VMEM(consts[1].shape[::-1], bf),
            pltpu.VMEM(consts[5].shape[::-1], bf),
            pltpu.VMEM(consts[3].shape[::-1], bf),
            pltpu.VMEM((points, lanes), bf),
            pltpu.VMEM((points, lanes), bf),
            pltpu.VMEM((extent, width + 2 * AMBIT), bf),
            pltpu.VMEM((2, AMBIT, width), bf),
            pltpu.VMEM((2, tile, AMBIT), bf),
            pltpu.VMEM((4, AMBIT, AMBIT), bf),
            pltpu.SemaphoreType.DMA((5 + len(consts),)),
        ]
        + [pltpu.SemaphoreType.DMA((10,))] * 4,
        compiler_params=pltpu.CompilerParams(
            collective_id=0, has_side_effects=True, vmem_limit_bytes=VMEM_LIMIT
        ),
    )(live, weights, mask, target, pupils, *consts)
    return mask - step_rate * gradient.astype(f32)


def solution(mesh):
    return jax.shard_map(
        partial(body, (mesh.shape["row"], mesh.shape["col"])),
        mesh=mesh,
        in_specs=(P("row", "col"), P("row", "col"), P("row", "col"), P(), P()),
        out_specs=P("row", "col"),
        check_vma=False,
    )
```
